32 devices in a mesh: track: 16 (over z, y, x), cam: 2 (over core).
Axes of the slice: x: 2, y: 2, z: 4, core: 2. Of those that a mesh axis runs over, the one named last changes fastest.
Arguments:
- omega: bfloat16 [32, 9, 4096], P(None, None, ('track', 'cam')), may hold values from -6 to 6
- u_blocks: float32 [9, 9, 4096], P(None, None, ('track', 'cam')), may hold values from -5.4 to 36, as said below
- w_blocks: bfloat16 [9, 3, 16384], P(None, None, ('track', 'cam')), may hold values from -1.796875 to 1.796875
- v_inverse: float32 [3, 3, 4096], P(None, None, ('track', 'cam')), may hold values from -0.6 to 1.5, as said below
- obs_camera: int32 [16384], P(('track', 'cam')), may hold values from 0 to 4095, as said below
- obs_track: int32 [16384], P(('track', 'cam')), may hold values from 0 to 31, as said below
- obs_mask: int32 [16384], P(('track', 'cam')), may hold values from 0 to 1, as said below
Outputs:
- sketch: float32 [32, 9, 4096], P(None, None, ('track', 'cam'))
- basis: float32 [32, 9, 4096], P(None, None, ('track', 'cam'))
- factor: float32 [32, 32], replicated
The draws below stay inside these ranges and needn't reach their ends.
Inputs may be any that keep to these rules, and one draw needn't show every extreme that they name: `obs_camera`: cameras c * 128 to (c + 1) * 128 - 1 belong to device c (track slower). Among one device's 512 observations, padding included, at most 32 name cameras of any one device, and exactly 32 name those of some device. `obs_track`: in each aligned block of 128 observations, slots 0 to 31 each hold one track of 2 to 4 consecutive observations from the block's start, in rising order; the padding after them carries slot 31. `obs_mask`: 1 on the observations of tracks, 0 on the padding at the end of each block. `u_blocks`: each block is symmetric. `v_inverse`: each block is symmetric positive definite.
All inputs are finite; a program needn't handle non-finite values.
Results may differ from the reference program's by a relative error of at most 0.00095.
Values may be sent and summed in bfloat16 or wider, within the bound.
A program may use at most 64 MiB of HBM per device.

```python
import math
import jax
import jax.numpy as jnp
from jax import lax

CAM_PARAMS = 9
COLS = 32
BLK_OBS = 128
TRK_BLK = 32
CAM_DEV = 128
OBS_DEV = 512
CAMS = 4096
OBS = 16384
TRACKS = 4096


def track_layout(key):
    blocks = OBS // BLK_OBS
    lengths = jax.random.randint(key, (blocks, TRK_BLK), 2, 5)
    ends = jnp.cumsum(lengths, axis=1)
    position = jnp.arange(BLK_OBS, dtype=jnp.int32)
    slot_ids = jnp.sum((position[None, :, None] >= ends[:, None, :]).astype(jnp.int32), axis=2)
    live_ids = (slot_ids < TRK_BLK).astype(jnp.int32)
    slot_ids = jnp.minimum(slot_ids, TRK_BLK - 1)
    return (slot_ids.reshape(-1).astype(jnp.int32), live_ids.reshape(-1))


def draw_obs_track(key, part):
    return track_layout(jax.random.fold_in(key, 11))[0]


def draw_obs_mask(key, part):
    return track_layout(jax.random.fold_in(key, 11))[1]


def draw_obs_camera(key, part):
    device_count = OBS // OBS_DEV
    capacity = max(2, 2 * OBS_DEV // device_count)
    slot_total = device_count * capacity

    def one_device(device_key):
        keys = jax.random.split(device_key, 5)
        heat = jax.random.randint(keys[0], (device_count,), 0, 4)
        full_owner = jax.random.randint(keys[1], (), 0, device_count)
        owner_of = jnp.arange(slot_total, dtype=jnp.int32) // capacity
        score = jax.random.randint(keys[2], (slot_total,), 0, 65536) + heat[owner_of] * 16384
        score = jnp.where(owner_of == full_owner, score + 1048576, score)
        picked = jnp.argsort(-score, stable=True)[:OBS_DEV]
        cameras = owner_of[picked] * CAM_DEV + jax.random.randint(keys[3], (OBS_DEV,), 0, CAM_DEV)
        return cameras[jax.random.permutation(keys[4], OBS_DEV)]
    return jax.vmap(one_device)(jax.random.split(key, device_count)).reshape(-1).astype(jnp.int32)


def draw_u_blocks(key, part):
    keys = jax.random.split(key, 2)
    cam_index = jnp.arange(CAMS, dtype=jnp.float32)
    growth = 2.0
    scaling = 1.0 + growth * cam_index / (CAMS - 1)
    diagonal = jax.random.uniform(keys[0], (9, CAMS), jnp.float32, 2.0, 4.0)
    rough = jax.random.uniform(keys[1], (9, 9, CAMS), jnp.float32, -0.6, 0.6)
    symmetric = 0.5 * (rough + rough.transpose(1, 0, 2))
    identity = jnp.eye(9, dtype=jnp.float32)[:, :, None]
    blocks = symmetric * (1.0 - identity) + identity * diagonal[:, None, :]
    return (blocks * scaling[None, None, :]).astype(jnp.float32)


def draw_v_inverse(key, part):
    keys = jax.random.split(key, 2)
    low_end, high_end = (0.3, 1.0)
    diagonal = jnp.exp(jax.random.uniform(keys[0], (3, TRACKS), jnp.float32, math.log(low_end), math.log(high_end)))
    rough = jax.random.uniform(keys[1], (3, 3, TRACKS), jnp.float32, -1.0, 1.0)
    symmetric = 0.5 * (rough + rough.transpose(1, 0, 2))
    root_diag = jnp.sqrt(diagonal)
    coupling = 0.4 * symmetric * root_diag[:, None, :] * root_diag[None, :, :]
    identity = jnp.eye(3, dtype=jnp.float32)[:, :, None]
    return (coupling * (1.0 - identity) + identity * diagonal[:, None, :]).astype(jnp.float32)


def shard_levels(rng, shape, pieces, smallest, high):
    def one(axis_at, blocks):
        draws = jax.random.uniform(jax.random.fold_in(jax.random.fold_in(rng, 6), axis_at), (blocks,), jnp.float32, smallest / len(pieces), high / len(pieces))
        return jnp.repeat(jnp.exp(draws), shape[axis_at] // blocks).reshape((-1,) + (1,) * (len(shape) - axis_at - 1))

    loudness = one(*pieces[0])
    for cut in pieces[1:]:
        loudness = loudness * one(*cut)
    return loudness


def noise(rng, dims, width, most, shards=(), held_as=jnp.bfloat16):
    entries = jax.random.normal(rng, dims, jnp.float32) * width
    if len(shards) > 0:
        entries = shard_levels(rng, dims, shards, -0.22, 0.18) * entries
    return jnp.clip(entries, min=-most, max=most).astype(held_as)


def setup_inputs(seed: int = 0) -> dict:
    key_list = jax.random.split(jax.random.key(seed), 8)
    omega = noise(key_list[0], (COLS, CAM_PARAMS, CAMS), 1.0, 6.0, ((2, 32),))
    u_blocks = draw_u_blocks(jax.random.fold_in(key_list[7], 71), 0)
    w_blocks = noise(key_list[2], (CAM_PARAMS, 3, OBS), 0.3, 1.796875, ((2, 32),))
    v_inverse = draw_v_inverse(jax.random.fold_in(key_list[7], 71), 0)
    obs_camera = draw_obs_camera(jax.random.fold_in(key_list[7], 71), 0)
    obs_track = draw_obs_track(jax.random.fold_in(key_list[7], 71), 0)
    obs_mask = draw_obs_mask(jax.random.fold_in(key_list[7], 71), 0)
    return {"omega": omega, "u_blocks": u_blocks, "w_blocks": w_blocks, "v_inverse": v_inverse, "obs_camera": obs_camera, "obs_track": obs_track, "obs_mask": obs_mask}


HIGH = lax.Precision.HIGHEST

def eliminate(gathered, weight, inverse, slot_ids, live_ids):
    live_mask = live_ids.astype(jnp.float32)
    track_ids = jnp.arange(OBS_DEV, dtype=jnp.int32) // BLK_OBS * TRK_BLK + slot_ids
    weight_f = weight.astype(jnp.float32)
    projected = jnp.einsum('mio,mco->ico', weight_f, gathered.astype(jnp.float32), precision=HIGH) * live_mask
    track_sum = jax.ops.segment_sum(projected.transpose(2, 0, 1), track_ids, num_segments=OBS_DEV // BLK_OBS * TRK_BLK)
    solved = jnp.einsum('ijt,tjc->tic', inverse, track_sum, precision=HIGH)
    spread = solved[track_ids]
    returned = jnp.einsum('mio,oic->mco', weight_f, spread, precision=HIGH) * live_mask
    return returned.astype(jnp.bfloat16)

def reference(omega, u_blocks, w_blocks, v_inverse, obs_camera, obs_track, obs_mask):
    device_count = OBS // OBS_DEV
    tracks_dev = OBS_DEV // BLK_OBS * TRK_BLK
    weights = w_blocks.reshape(9, 3, device_count, OBS_DEV).transpose(2, 0, 1, 3)
    inverses = v_inverse.reshape(3, 3, device_count, tracks_dev).transpose(2, 0, 1, 3)
    cameras = obs_camera.reshape(device_count, OBS_DEV)
    slots = obs_track.reshape(device_count, OBS_DEV)
    masks = obs_mask.reshape(device_count, OBS_DEV)

    def visit_device(accumulated, device_part):
        weight, inverse, camera, slot_ids, live_ids = device_part
        gathered = jnp.take(omega, camera, axis=2).transpose(1, 0, 2)
        returned = eliminate(gathered, weight, inverse, slot_ids, live_ids)
        accumulated = accumulated.at[:, :, camera].add(returned.astype(jnp.float32).transpose(1, 0, 2))
        return (accumulated, None)
    accumulated, _ = lax.scan(visit_device, jnp.zeros(omega.shape, jnp.float32), (weights, inverses, cameras, slots, masks))
    own_term = jnp.einsum('mnk,jnk->jmk', u_blocks.astype(jnp.float32), omega.astype(jnp.float32), precision=HIGH)
    sketch = own_term - accumulated
    flat_rows = sketch.reshape(sketch.shape[0], -1)
    gram_matrix = jnp.dot(flat_rows.astype(jnp.float32), flat_rows.T.astype(jnp.float32), precision=HIGH, preferred_element_type=jnp.float32)
    lower_factor = jnp.linalg.cholesky(gram_matrix / flat_rows.shape[1])
    basis_rows = jax.scipy.linalg.solve_triangular(lower_factor, flat_rows, lower=True).reshape(sketch.shape)
    return (sketch, basis_rows, lower_factor.T)
```

```python
import functools

import jax
import jax.numpy as jnp
from jax import lax
from jax.experimental import pallas as pl
from jax.experimental.pallas import tpu as pltpu
from jax.sharding import PartitionSpec as P

BLK_OBS = 128
TRK_BLK = 32
LANES = 128
STRIP = 8
CHUNK = 512

HIGH = lax.Precision.HIGHEST
MESH = pl.DeviceIdType.MESH
NT = (((1,), (1,)), ((), ()))
F32 = jnp.float32
BF16 = jnp.bfloat16

ASK, ASK_FAR, TABLE, SUM, SUM_FAR, BACK, BACK_FAR, GRAM = range(8)


def dot(left, right, precision=None):
    return jnp.dot(left, right, precision=precision, preferred_element_type=F32)


def dot_nt(left, right, precision=None):
    return lax.dot_general(left, right, NT, precision=precision, preferred_element_type=F32)


def one_hot(condition):
    return jnp.where(condition, 1.0, 0.0).astype(BF16)


def rows_iota(shape):
    return lax.broadcasted_iota(jnp.int32, shape, 0)


def lanes_iota(shape):
    return lax.broadcasted_iota(jnp.int32, shape, 1)


def repeat(count, body):
    if count == 1:
        body(0)
    else:
        pl.loop(0, count)(body)


def kernel(
    sizes,
    omega_hbm, u_hbm, w_hbm, v_hbm, camera_hbm, track_hbm, mask_hbm,
    sketch_ref, packed_ref,
    send1, recv1, recv1_far, send2, recv2, send3, recv3, gsend, grecv, far_table,
    fields, to_track, wide, pick, far_wide, far_pick, own, incoming, sum_ref,
    send_sems, recv_sems,
    omega_ref, u_ref, w_ref, v_ref, camera_ref, track_ref, mask_ref, load_sems,
):
    track_count, cam_count, params, columns, rows, groups, span = sizes
    devices = track_count * cam_count
    half = devices // 2
    cam_width = omega_ref.shape[1]
    obs_count = camera_ref.shape[1]
    tracks = v_ref.shape[2]
    part_rows = span * rows
    chunk = groups * part_rows
    chunks = half // span
    me = lax.axis_index("track") * cam_count + lax.axis_index("cam")
    side = me // half
    place_at = me - side * half
    home = side * half
    away = half - home

    def where(device):
        return (device // cam_count, lax.rem(device, cam_count))

    def turned_place(turn):
        return lax.rem(place_at + turn, half)

    loads = [
        pltpu.make_async_copy(source, target, load_sems.at[index])
        for index, (source, target) in enumerate(
            [
                (camera_hbm, camera_ref),
                (track_hbm, track_ref),
                (mask_hbm, mask_ref),
                (w_hbm, w_ref),
                (omega_hbm, omega_ref),
                (u_hbm, u_ref),
                (v_hbm, v_ref),
            ]
        )
    ]
    for load in loads:
        load.start()

    barrier = pltpu.get_barrier_semaphore()
    pl.semaphore_signal(
        barrier, inc=1, device_id=where(away + place_at), device_id_type=MESH
    )

    @pl.loop(1, half)
    def _(turn):
        pl.semaphore_signal(
            barrier, inc=1, device_id=where(home + turned_place(turn)), device_id_type=MESH
        )

    def remote(index, src, dst, device):
        return pltpu.make_async_remote_copy(
            src_ref=src,
            dst_ref=dst,
            send_sem=send_sems.at[index],
            recv_sem=recv_sems.at[index],
            device_id=where(device),
            device_id_type=MESH,
        )

    def to_home(index, src, dst):
        @pl.loop(1, half)
        def _(turn):
            other = turned_place(turn)
            remote(index, src.at[other], dst.at[place_at], home + other).start()

        pltpu.make_async_copy(src.at[place_at], dst.at[place_at], recv_sems.at[index]).start()

    def to_away(index, src, dst):
        @pl.loop(0, half)
        def _(turn):
            other = turned_place(turn)
            remote(index, src(other), dst.at[place_at], away + other).start()

    def arrive(index, dst):
        pltpu.make_async_copy(dst, dst, recv_sems.at[index]).wait()

    def sent(index, part):
        pltpu.make_async_copy(part, part, send_sems.at[index]).wait()

    eye = one_hot(rows_iota((LANES, LANES)) == lanes_iota((LANES, LANES)))

    def pack(part, values, dst, at=0):
        for index in range(values.shape[0] // columns):
            block = values[index * columns : (index + 1) * columns]
            pieces = [block[:, g * part_rows : (g + 1) * part_rows] for g in range(groups)]
            if groups * columns < LANES:
                pieces.append(jnp.zeros((LANES - groups * columns, part_rows), F32))
            turned = jnp.concatenate(pieces, axis=0).T.reshape(span, rows, LANES)
            low = at + index * rows
            dst[pl.ds(part * span, span), low : low + rows] = turned.astype(BF16)

    def unpack(part, src, at, count):
        blocks = []
        for index in range(count):
            low = at + index * rows
            block = src[pl.ds(part * span, span), low : low + rows]
            turned = dot_nt(eye, block.reshape(part_rows, LANES))
            blocks.append(
                jnp.concatenate(
                    [turned[g * columns : (g + 1) * columns] for g in range(groups)], axis=1
                )
            )
        return jnp.concatenate(blocks, axis=0)

    with jax.named_scope("place"):
        for load in loads[:4]:
            load.wait()
        camera = camera_ref[...]
        owner = camera // cam_width
        local = camera - owner * cam_width
        owner = owner - home
        owner = jnp.where(owner < 0, owner + devices, owner)
        track_id = lanes_iota((1, obs_count)) // BLK_OBS * TRK_BLK + track_ref[...]
        live = mask_ref[...].astype(F32)
        fields[...] = jnp.zeros_like(fields)
        for row in range(params):
            fields[3 * row : 3 * row + 3, :] = w_ref[row].astype(F32) * live
        high = local // 256
        fields[3 * params : 3 * params + 1, :] = high.astype(F32)
        fields[3 * params + 1 : 3 * params + 2, :] = (local - high * 256).astype(F32)
        owned = one_hot(rows_iota((devices, obs_count)) == owner)
        earlier = one_hot(rows_iota((obs_count, obs_count)) < lanes_iota((obs_count, obs_count)))
        ranks = dot(owned, earlier)
        rank = jnp.sum(ranks * owned.astype(F32), axis=0, keepdims=True).astype(jnp.int32)
        group = jnp.zeros_like(rank)
        for g in range(1, groups):
            group += jnp.where(rank >= g * rows, 1, 0)
        offset = group * part_rows + rank - group * rows
        member = one_hot(rows_iota((tracks, obs_count)) == track_id)
        table = jnp.concatenate([fields[...].astype(BF16), member], axis=0)

        for far in range(2):

            def place(part):
                nearby = owner - far * half - part * span
                inside = jnp.logical_and(nearby >= 0, nearby < span)
                slot = jnp.where(inside, nearby * rows + offset, -1)
                slots = one_hot(rows_iota((chunk, obs_count)) == slot)
                placed = dot_nt(table, slots)
                pack(part, placed[:columns], send1, far * rows)
                to_track[far, part] = placed[columns:].astype(BF16)

            repeat(chunks, place)

    with jax.named_scope("barrier"):
        loads[4].wait()
        pl.semaphore_wait(barrier, half)
    table_copy = remote(TABLE, omega_ref, far_table, away + place_at)
    table_copy.start()
    to_home(ASK, send1, recv1)

    with jax.named_scope("own"):
        for load in loads[5:]:
            load.wait()
        for row in range(params):
            total = jnp.zeros((columns, cam_width), F32)
            for col in range(params):
                total += u_ref[row, col : col + 1, :] * omega_ref[
                    col * columns : (col + 1) * columns, :
                ].astype(F32)
            own[row * columns : (row + 1) * columns, :] = total
        incoming[...] = jnp.zeros_like(incoming)
        sum_ref[...] = jnp.zeros_like(sum_ref)

    def read_request(part, src, at, wide_to, pick_to):
        turned = unpack(part, src, at, 1)
        wide_to[part] = turned
        number = turned[3 * params : 3 * params + 1] * 256.0 + turned[
            3 * params + 1 : 3 * params + 2
        ]
        pick_to[part] = one_hot(rows_iota((cam_width, chunk)) == number.astype(jnp.int32))

    def project(part, cameras, weights, chosen, dst):
        gathered = dot(cameras[...], chosen[part])
        turned = weights[part]
        pieces = []
        for comp in range(3):
            total = jnp.zeros((columns, chunk), F32)
            for row in range(params):
                at = row * 3 + comp
                total += turned[at : at + 1] * gathered[row * columns : (row + 1) * columns]
            pieces.append(total)
        pack(part, jnp.concatenate(pieces, axis=0), dst)

    with jax.named_scope("wait_ask"):
        arrive(ASK, recv1)
    with jax.named_scope("project"):
        repeat(chunks, lambda part: read_request(part, recv1, 0, wide.at[0], pick.at[0]))
        repeat(chunks, lambda part: project(part, omega_ref, wide.at[0], pick.at[0], send2.at[0]))
    to_home(SUM, send2.at[0], recv2.at[0])
    to_away(ASK_FAR, lambda other: send1.at[other, pl.ds(rows, rows)], recv1_far)
    with jax.named_scope("read_far"):
        repeat(chunks, lambda part: read_request(part, recv1, rows, far_wide, far_pick))
    with jax.named_scope("wait_table"):
        arrive(TABLE, far_table)
    with jax.named_scope("project_far"):
        repeat(chunks, lambda part: project(part, far_table, far_wide, far_pick, send2.at[1]))
    to_home(SUM_FAR, send2.at[1], recv2.at[1])

    def collect(far, part):
        values = unpack(part, recv2.at[far], 0, 3).astype(BF16)
        sum_ref[...] += dot_nt(values, to_track[far, part])

    with jax.named_scope("wait_sum"):
        arrive(SUM, recv2.at[0])
    with jax.named_scope("collect"):
        repeat(chunks, lambda part: collect(0, part))
    with jax.named_scope("wait_sum_far"):
        arrive(SUM_FAR, recv2.at[1])
    with jax.named_scope("collect_far"):
        repeat(chunks, lambda part: collect(1, part))
        pieces = []
        for row in range(3):
            total = jnp.zeros((columns, tracks), F32)
            for col in range(3):
                total += v_ref[row, col : col + 1, :] * sum_ref[
                    col * columns : (col + 1) * columns
                ]
            pieces.append(total)
        solved = jnp.concatenate(pieces, axis=0).astype(BF16)
        repeat(
            chunks, lambda part: pack(part, dot(solved, to_track[1, part]), send3.at[1])
        )
    to_away(BACK_FAR, lambda other: send3.at[1, other], recv3.at[1])
    with jax.named_scope("spread"):
        repeat(
            chunks, lambda part: pack(part, dot(solved, to_track[0, part]), send3.at[0])
        )
    to_home(BACK, send3.at[0], recv3.at[0])
    with jax.named_scope("read_ask_far"):
        arrive(ASK_FAR, recv1_far)
        repeat(chunks, lambda part: read_request(part, recv1_far, 0, wide.at[1], pick.at[1]))

    def gather_back(far, part):
        turned = unpack(part, recv3.at[far], 0, 3)
        weights = wide[far, part]
        pieces = []
        for row in range(params):
            total = jnp.zeros((columns, chunk), F32)
            for comp in range(3):
                at = row * 3 + comp
                total += weights[at : at + 1] * turned[comp * columns : (comp + 1) * columns]
            pieces.append(total)
        contribution = jnp.concatenate(pieces, axis=0).astype(BF16)
        incoming[...] += dot_nt(contribution, pick[far, part])

    with jax.named_scope("wait_back"):
        arrive(BACK, recv3.at[0])
    with jax.named_scope("gather"):
        repeat(chunks, lambda part: gather_back(0, part))
    with jax.named_scope("wait_back_far"):
        arrive(BACK_FAR, recv3.at[1])
    with jax.named_scope("gather_far"):
        repeat(chunks, lambda part: gather_back(1, part))

        sketch = own[...] - incoming[...]
        sketch_ref[...] = sketch
        flat = jnp.concatenate(
            [sketch[row * columns : (row + 1) * columns] for row in range(params)], axis=1
        )
        gram = dot_nt(flat, flat, HIGH)
        folds = LANES // columns
        tall = columns // folds
        gsend[...] = jnp.concatenate(
            [gram[part * tall : (part + 1) * tall] for part in range(folds)], axis=1
        )

    @pl.loop(1, devices)
    def _(turn):
        remote(GRAM, gsend, grecv.at[me], lax.rem(me + turn, devices)).start()

    pltpu.make_async_copy(gsend, grecv.at[me], recv_sems.at[GRAM]).start()
    with jax.named_scope("wait_gram"):
        arrive(GRAM, grecv)
    packed_ref[...] = jnp.sum(grecv[...], axis=0)

    most = pl.ds(0, half - 1)
    sent(ASK, recv1.at[most])
    sent(ASK_FAR, recv1_far)
    sent(TABLE, far_table)
    sent(SUM, recv2.at[0, most])
    sent(SUM_FAR, recv2.at[1, most])
    sent(BACK, recv3.at[0, most])
    sent(BACK_FAR, recv3.at[1])
    sent(GRAM, grecv.at[pl.ds(0, devices - 1)])


def finish(
    sizes,
    sketch_ref, packed_ref,
    sketch_hbm, basis_hbm, factor_hbm,
    basis_ref, factor_ref, sems,
):
    params, columns, height = sizes
    cam_width = sketch_ref.shape[1]
    sketch_copy = pltpu.make_async_copy(sketch_ref, sketch_hbm, sems.at[0])
    sketch_copy.start()
    with jax.named_scope("eliminate"):
        folds = LANES // columns
        packed = packed_ref[...]
        gram = jnp.concatenate(
            [packed[:, part * columns : (part + 1) * columns] for part in range(folds)], axis=0
        ) / height
        strips = columns // STRIP
        unit = jnp.where(
            rows_iota((columns, columns)) == lanes_iota((columns, columns)), 1.0, 0.0
        )
        both = jnp.concatenate([unit, gram], axis=1)
        work = [both[s * STRIP : (s + 1) * STRIP] for s in range(strips)]
        row_ids = rows_iota((STRIP, 1))
        roots = [jnp.zeros((STRIP, LANES), F32) for _ in range(strips)]
        for base in range(strips):
            panel = [
                [
                    jnp.broadcast_to(
                        work[s][:, columns + base * STRIP + j : columns + base * STRIP + j + 1],
                        (STRIP, LANES),
                    )
                    for s in range(strips)
                ]
                for j in range(STRIP)
            ]
            for j in range(STRIP):
                pivot = panel[j][base][j : j + 1]
                inverse = 1.0 / pivot
                roots[base] = jnp.where(row_ids == j, lax.rsqrt(pivot), roots[base])
                for s in range(base, strips):
                    scale = jnp.where(row_ids > j, inverse, 0.0) if s == base else inverse
                    work[s] = work[s] - (panel[j][s] * scale)[:, : 2 * columns] * work[base][
                        j : j + 1
                    ]
                    for later in range(j + 1, STRIP):
                        panel[later][s] = panel[later][s] - (
                            panel[j][s] * panel[later][base][j : j + 1]
                        ) * scale
        done = jnp.concatenate(
            [work[s] * roots[s][:, : 2 * columns] for s in range(strips)], axis=0
        )
        inverse = done[:, :columns]
        on_upper = rows_iota((columns, columns)) <= lanes_iota((columns, columns))
        factor_ref[...] = jnp.where(on_upper, done[:, columns:], 0.0)
    factor_copy = pltpu.make_async_copy(factor_ref, factor_hbm, sems.at[1])
    factor_copy.start()
    with jax.named_scope("basis"):
        flat = jnp.concatenate(
            [sketch_ref[row * columns : (row + 1) * columns] for row in range(params)], axis=1
        )
        basis = dot(inverse, flat, HIGH)
        for row in range(params):
            basis_ref[row * columns : (row + 1) * columns, :] = basis[
                :, row * cam_width : (row + 1) * cam_width
            ]
    basis_copy = pltpu.make_async_copy(basis_ref, basis_hbm, sems.at[2])
    basis_copy.start()
    with jax.named_scope("write"):
        sketch_copy.wait()
        factor_copy.wait()
        basis_copy.wait()


def on_device(omega, u_blocks, w_blocks, v_inverse, obs_camera, obs_track, obs_mask):
    track_count = lax.axis_size("track")
    cam_count = lax.axis_size("cam")
    devices = track_count * cam_count
    half = devices // 2
    columns, params, cam_width = omega.shape
    obs_count = obs_camera.shape[0]
    tracks = v_inverse.shape[2]
    capacity = max(2, 2 * obs_count // devices)
    rows = -(-capacity // (LANES // columns) // 8) * 8
    groups = -(-capacity // rows)
    span = half
    while span * rows * groups > CHUNK and span % 2 == 0:
        span //= 2
    chunk = span * rows * groups
    chunks = half // span

    table = omega.transpose(1, 0, 2).reshape(params * columns, cam_width)
    line = (1, obs_count)
    operands = (
        table,
        u_blocks,
        w_blocks,
        v_inverse,
        obs_camera.reshape(line),
        obs_track.reshape(line),
        obs_mask.reshape(line),
    )
    sizes = (track_count, cam_count, params, columns, rows, groups, span)
    message = pltpu.VMEM((2, half, 3 * rows, LANES), BF16)
    tall = columns * columns // LANES
    wide_shape = (chunks, columns, chunk)
    pick_shape = (chunks, cam_width, chunk)
    whole = jax.ShapeDtypeStruct((params * columns, cam_width), F32)
    square = jax.ShapeDtypeStruct((columns, columns), F32)
    in_vmem = pl.BlockSpec(memory_space=pltpu.VMEM)
    anywhere = pl.BlockSpec(memory_space=pl.ANY)
    sketch, packed = pl.pallas_call(
        functools.partial(kernel, sizes),
        out_shape=(
            pltpu.VMEM((params * columns, cam_width), F32),
            pltpu.VMEM((tall, LANES), F32),
        ),
        in_specs=[anywhere] * 7,
        out_specs=(in_vmem,) * 2,
        scratch_shapes=[
            pltpu.VMEM((half, 2 * rows, LANES), BF16),
            pltpu.VMEM((half, 2 * rows, LANES), BF16),
            pltpu.VMEM((half, rows, LANES), BF16),
        ]
        + [message] * 4
        + [
            pltpu.VMEM((tall, LANES), F32),
            pltpu.VMEM((devices, tall, LANES), F32),
            pltpu.VMEM((params * columns, cam_width), BF16),
            pltpu.VMEM((columns, obs_count), F32),
            pltpu.VMEM((2, chunks, tracks, chunk), BF16),
            pltpu.VMEM((2,) + wide_shape, F32),
            pltpu.VMEM((2,) + pick_shape, BF16),
            pltpu.VMEM(wide_shape, F32),
            pltpu.VMEM(pick_shape, BF16),
            pltpu.VMEM((params * columns, cam_width), F32),
            pltpu.VMEM((params * columns, cam_width), F32),
            pltpu.VMEM((3 * columns, tracks), F32),
            pltpu.SemaphoreType.DMA((8,)),
            pltpu.SemaphoreType.DMA((8,)),
        ]
        + [pltpu.VMEM(array.shape, array.dtype) for array in operands]
        + [pltpu.SemaphoreType.DMA((len(operands),))],
        compiler_params=pltpu.CompilerParams(collective_id=0, has_side_effects=True),
    )(*operands)
    sketch, basis, factor = pl.pallas_call(
        functools.partial(finish, (params, columns, params * cam_width * devices)),
        out_shape=(whole, whole, square),
        in_specs=[in_vmem] * 2,
        out_specs=(anywhere,) * 3,
        scratch_shapes=[
            pltpu.VMEM((params * columns, cam_width), F32),
            pltpu.VMEM((columns, columns), F32),
            pltpu.SemaphoreType.DMA((3,)),
        ],
    )(*(pltpu.with_memory_space_constraint(x, pltpu.VMEM) for x in (sketch, packed)))

    def unfold(array):
        return array.reshape(params, columns, cam_width).transpose(1, 0, 2)

    return (unfold(sketch), unfold(basis), factor)


def solution(mesh):
    spread = P(None, None, ("track", "cam"))
    flat = P(("track", "cam"))
    return jax.shard_map(
        on_device,
        mesh=mesh,
        in_specs=(spread,) * 4 + (flat,) * 3,
        out_specs=(spread, spread, P()),
        check_vma=False,
    )
```

```python
import functools

import jax
import jax.numpy as jnp
from jax import lax
from jax.experimental import pallas as pl
from jax.experimental.pallas import tpu as pltpu
from jax.sharding import PartitionSpec as P

BLK_OBS = 128
TRK_BLK = 32
LANES = 128
STRIP = 8
CHUNK = 512
UNROLL = 32

HIGH = lax.Precision.HIGHEST
LOGICAL = pl.DeviceIdType.LOGICAL
NT = (((1,), (1,)), ((), ()))
F32 = jnp.float32
BF16 = jnp.bfloat16

ASK, ASK_FAR, TABLE, SUM, SUM_FAR, BACK, BACK_FAR, GRAM = range(8)


def dot(left, right, precision=None):
    return jnp.dot(left, right, precision=precision, preferred_element_type=F32)


def dot_nt(left, right, precision=None):
    return lax.dot_general(left, right, NT, precision=precision, preferred_element_type=F32)


def one_hot(condition):
    return jnp.where(condition, 1.0, 0.0).astype(BF16)


def rows_iota(shape):
    return lax.broadcasted_iota(jnp.int32, shape, 0)


def lanes_iota(shape):
    return lax.broadcasted_iota(jnp.int32, shape, 1)


def turns(first, count, body):
    if count - first <= UNROLL:
        for turn in range(first, count):
            body(turn)
    else:
        pl.loop(first, count)(body)


def repeat(count, body):
    if count == 1:
        body(0)
    else:
        pl.loop(0, count)(body)


def fold(gram):
    columns = gram.shape[0]
    middle = columns // 2
    folds = LANES // columns
    tall = middle // folds
    top, bottom = gram[:middle], gram[middle:]
    first, second = [], []
    for k in range(folds):
        first.append(top[k * tall : (k + 1) * tall])
        piece = bottom[k * tall : (k + 1) * tall]
        second += [piece[:, middle:], piece[:, :middle]]
    lane = lanes_iota((tall, LANES))
    row = rows_iota((tall, LANES)) + lane // columns * tall
    packed = jnp.where(
        lax.rem(lane, columns) >= row,
        jnp.concatenate(first, axis=1),
        jnp.concatenate(second, axis=1),
    )
    shape = (middle, columns)
    on_diagonal = lanes_iota(shape) == rows_iota(shape) + middle
    diagonal = jnp.sum(jnp.where(on_diagonal, bottom, 0.0), axis=0, keepdims=True)
    diagonal = jnp.concatenate([diagonal, jnp.zeros((1, LANES - columns), F32)], axis=1)
    return jnp.concatenate([packed, diagonal], axis=0)


def unfold_gram(packed, columns):
    middle = columns // 2
    folds = LANES // columns
    tall = middle // folds
    both = jnp.concatenate(
        [packed[:tall, k * columns : (k + 1) * columns] for k in range(folds)], axis=0
    )
    gap = jnp.zeros((tall, middle), F32)
    moved = jnp.concatenate(
        [
            jnp.concatenate([gap, packed[:tall, k * columns : k * columns + middle]], axis=1)
            for k in range(folds)
        ],
        axis=0,
    )
    shape = (middle, columns)
    row, lane = rows_iota(shape), lanes_iota(shape)
    top = jnp.where(lane >= row, both, 0.0)
    bottom = jnp.where(lane < row + middle, moved, 0.0)
    bottom += jnp.where(lane == row + middle, packed[tall : tall + 1, :columns], 0.0)
    half = jnp.concatenate([top, bottom], axis=0)
    square = (columns, columns)
    wide = jnp.concatenate([half, jnp.zeros((columns, LANES - columns), F32)], axis=1)
    turned = jnp.concatenate([wide] + [jnp.zeros((LANES - columns, LANES), F32)], axis=0).T
    turned = turned[:columns, :columns]
    return half + jnp.where(lanes_iota(square) == rows_iota(square), 0.0, turned)


def kernel(
    sizes,
    omega_hbm, u_hbm, w_hbm, v_hbm, camera_hbm, track_hbm, mask_hbm,
    sketch_ref, packed_ref,
    send1, recv1, recv1_far, send2, recv2, send3, recv3, gsend, grecv, far_table,
    fields, to_track, wide, pick, far_wide, far_pick, own, incoming, sum_ref,
    send_sems, recv_sems,
    omega_ref, u_ref, w_ref, v_ref, camera_ref, track_ref, mask_ref, load_sems,
):
    track_count, cam_count, params, columns, rows, groups, span = sizes
    devices = track_count * cam_count
    half = devices // 2
    cam_width = omega_ref.shape[1]
    obs_count = camera_ref.shape[1]
    tracks = v_ref.shape[2]
    part_rows = span * rows
    chunk = groups * part_rows
    chunks = half // span
    me = lax.axis_index("track") * cam_count + lax.axis_index("cam")
    side = me // half
    place_at = me - side * half
    home = side * half
    away = half - home

    def wrapped(start, turn, count):
        place = start + turn
        return jnp.where(place >= count, place - count, place)

    barrier = pltpu.get_barrier_semaphore()

    def greet(device):
        pl.semaphore_signal(barrier, inc=1, device_id=device, device_id_type=LOGICAL)

    turns(1, half, lambda turn: greet(home + wrapped(place_at, turn, half)))
    greet(away + place_at)

    loads = [
        pltpu.make_async_copy(source, target, load_sems.at[index])
        for index, (source, target) in enumerate(
            [
                (camera_hbm, camera_ref),
                (track_hbm, track_ref),
                (mask_hbm, mask_ref),
                (w_hbm, w_ref),
                (omega_hbm, omega_ref),
                (u_hbm, u_ref),
                (v_hbm, v_ref),
            ]
        )
    ]
    for load in loads:
        load.start()

    def remote(index, src, dst, device):
        return pltpu.make_async_remote_copy(
            src_ref=src,
            dst_ref=dst,
            send_sem=send_sems.at[index],
            recv_sem=recv_sems.at[index],
            device_id=device,
            device_id_type=LOGICAL,
        )

    def to_home(index, src, dst):
        def send(turn):
            other = wrapped(place_at, turn, half)
            remote(index, src.at[other], dst.at[place_at], home + other).start()

        turns(1, half, send)
        pltpu.make_async_copy(src.at[place_at], dst.at[place_at], recv_sems.at[index]).start()

    far_first = lax.rem(place_at, half // 2) + (1 - side) * (half // 2)

    def to_away(index, src, dst):
        def send(turn):
            other = wrapped(far_first, turn, half)
            remote(index, src(other), dst.at[place_at], away + other).start()

        turns(0, half, send)

    def arrive(index, dst):
        pltpu.make_async_copy(dst, dst, recv_sems.at[index]).wait()

    def sent(index, part):
        pltpu.make_async_copy(part, part, send_sems.at[index]).wait()

    def pack(part, values, dst, at=0):
        for index in range(values.shape[0] // columns):
            block = values[index * columns : (index + 1) * columns]
            pieces = [block[:, g * part_rows : (g + 1) * part_rows] for g in range(groups)]
            if groups * columns < LANES:
                pieces.append(jnp.zeros((LANES - groups * columns, part_rows), F32))
            turned = jnp.concatenate(pieces, axis=0).T.reshape(span, rows, LANES)
            low = at + index * rows
            dst[pl.ds(part * span, span), low : low + rows] = turned.astype(BF16)

    def unpack(part, src, at, count):
        blocks = []
        for index in range(count):
            low = at + index * rows
            block = src[pl.ds(part * span, span), low : low + rows]
            turned = block.reshape(part_rows, LANES).astype(F32).T
            blocks.append(
                jnp.concatenate(
                    [turned[g * columns : (g + 1) * columns] for g in range(groups)], axis=1
                )
            )
        return jnp.concatenate(blocks, axis=0)

    with jax.named_scope("place"):
        for load in loads[:4]:
            load.wait()
        camera = camera_ref[...]
        owner = camera // cam_width
        local = camera - owner * cam_width
        owner = owner - home
        owner = jnp.where(owner < 0, owner + devices, owner)
        track_id = lanes_iota((1, obs_count)) // BLK_OBS * TRK_BLK + track_ref[...]
        live = mask_ref[...].astype(F32)
        fields[...] = jnp.zeros_like(fields)
        for row in range(params):
            fields[3 * row : 3 * row + 3, :] = w_ref[row].astype(F32) * live
        high = local // 256
        fields[3 * params : 3 * params + 1, :] = high.astype(F32)
        fields[3 * params + 1 : 3 * params + 2, :] = (local - high * 256).astype(F32)
        owned = one_hot(rows_iota((devices, obs_count)) == owner)
        earlier = one_hot(rows_iota((obs_count, obs_count)) < lanes_iota((obs_count, obs_count)))
        ranks = dot(owned, earlier)
        rank = jnp.sum(ranks * owned.astype(F32), axis=0, keepdims=True).astype(jnp.int32)
        group = jnp.zeros_like(rank)
        for g in range(1, groups):
            group += jnp.where(rank >= g * rows, 1, 0)
        offset = group * part_rows + rank - group * rows
        member = one_hot(rows_iota((tracks, obs_count)) == track_id)
        table = jnp.concatenate([fields[...].astype(BF16), member], axis=0)

        for far in range(2):

            def place(part):
                nearby = owner - far * half - part * span
                inside = jnp.logical_and(nearby >= 0, nearby < span)
                slot = jnp.where(inside, nearby * rows + offset, -1)
                slots = one_hot(rows_iota((chunk, obs_count)) == slot)
                placed = dot_nt(table, slots)
                pack(part, placed[:columns], send1, far * rows)
                to_track[far, part] = placed[columns:].astype(BF16)

            repeat(chunks, place)

    with jax.named_scope("barrier"):
        loads[4].wait()
        pl.semaphore_wait(barrier, half)
    table_copy = remote(TABLE, omega_ref, far_table, away + place_at)
    to_home(ASK, send1, recv1)
    table_copy.start()

    with jax.named_scope("own"):
        for load in loads[5:]:
            load.wait()
        for row in range(params):
            total = jnp.zeros((columns, cam_width), F32)
            for col in range(params):
                total += u_ref[row, col : col + 1, :] * omega_ref[
                    col * columns : (col + 1) * columns, :
                ].astype(F32)
            own[row * columns : (row + 1) * columns, :] = total
        incoming[...] = jnp.zeros_like(incoming)
        sum_ref[...] = jnp.zeros_like(sum_ref)

    def read_request(part, src, at, wide_to, pick_to):
        turned = unpack(part, src, at, 1)
        wide_to[part] = turned
        number = turned[3 * params : 3 * params + 1] * 256.0 + turned[
            3 * params + 1 : 3 * params + 2
        ]
        pick_to[part] = one_hot(rows_iota((cam_width, chunk)) == number.astype(jnp.int32))

    def project(part, cameras, weights, chosen, dst):
        gathered = dot(cameras[...], chosen[part])
        turned = weights[part]
        pieces = []
        for comp in range(3):
            total = jnp.zeros((columns, chunk), F32)
            for row in range(params):
                at = row * 3 + comp
                total += turned[at : at + 1] * gathered[row * columns : (row + 1) * columns]
            pieces.append(total)
        pack(part, jnp.concatenate(pieces, axis=0), dst)

    with jax.named_scope("wait_ask"):
        arrive(ASK, recv1)
    with jax.named_scope("project"):
        repeat(chunks, lambda part: read_request(part, recv1, 0, wide.at[0], pick.at[0]))
        repeat(chunks, lambda part: project(part, omega_ref, wide.at[0], pick.at[0], send2.at[0]))
    to_home(SUM, send2.at[0], recv2.at[0])
    with jax.named_scope("read_far"):
        repeat(chunks, lambda part: read_request(part, recv1, rows, far_wide, far_pick))
    with jax.named_scope("wait_table"):
        arrive(TABLE, far_table)
    with jax.named_scope("project_far"):
        repeat(chunks, lambda part: project(part, far_table, far_wide, far_pick, send2.at[1]))
    to_home(SUM_FAR, send2.at[1], recv2.at[1])
    to_away(ASK_FAR, lambda other: send1.at[other, pl.ds(rows, rows)], recv1_far)

    def collect(far, part):
        values = unpack(part, recv2.at[far], 0, 3).astype(BF16)
        sum_ref[...] += dot_nt(values, to_track[far, part])

    with jax.named_scope("wait_sum"):
        arrive(SUM, recv2.at[0])
    with jax.named_scope("collect"):
        repeat(chunks, lambda part: collect(0, part))
    with jax.named_scope("wait_sum_far"):
        arrive(SUM_FAR, recv2.at[1])
    with jax.named_scope("collect_far"):
        repeat(chunks, lambda part: collect(1, part))
        pieces = []
        for row in range(3):
            total = jnp.zeros((columns, tracks), F32)
            for col in range(3):
                total += v_ref[row, col : col + 1, :] * sum_ref[
                    col * columns : (col + 1) * columns
                ]
            pieces.append(total)
        solved = jnp.concatenate(pieces, axis=0).astype(BF16)
        repeat(
            chunks, lambda part: pack(part, dot(solved, to_track[1, part]), send3.at[1])
        )
    to_away(BACK_FAR, lambda other: send3.at[1, other], recv3.at[1])
    with jax.named_scope("spread"):
        repeat(
            chunks, lambda part: pack(part, dot(solved, to_track[0, part]), send3.at[0])
        )
    to_home(BACK, send3.at[0], recv3.at[0])
    with jax.named_scope("read_ask_far"):
        arrive(ASK_FAR, recv1_far)
        repeat(chunks, lambda part: read_request(part, recv1_far, 0, wide.at[1], pick.at[1]))

    def gather_back(far, part):
        turned = unpack(part, recv3.at[far], 0, 3)
        weights = wide[far, part]
        pieces = []
        for row in range(params):
            total = jnp.zeros((columns, chunk), F32)
            for comp in range(3):
                at = row * 3 + comp
                total += weights[at : at + 1] * turned[comp * columns : (comp + 1) * columns]
            pieces.append(total)
        contribution = jnp.concatenate(pieces, axis=0).astype(BF16)
        incoming[...] += dot_nt(contribution, pick[far, part])

    with jax.named_scope("wait_back"):
        arrive(BACK, recv3.at[0])
    with jax.named_scope("gather"):
        repeat(chunks, lambda part: gather_back(0, part))
    with jax.named_scope("wait_back_far"):
        arrive(BACK_FAR, recv3.at[1])
    with jax.named_scope("gather_far"):
        repeat(chunks, lambda part: gather_back(1, part))

        sketch = own[...] - incoming[...]
        sketch_ref[...] = sketch
        flat = jnp.concatenate(
            [sketch[row * columns : (row + 1) * columns] for row in range(params)], axis=1
        )
        head = flat.astype(BF16)
        rest = (flat - head.astype(F32)).astype(BF16)
        parts = jnp.concatenate([head, rest], axis=0)
        products = dot_nt(parts, head) + dot_nt(parts, rest)
        gram = products[:columns] + products[columns:]
        gsend[...] = fold(gram)

    def send_gram(turn):
        remote(GRAM, gsend, grecv.at[me], wrapped(me, turn, devices)).start()

    turns(1, devices, send_gram)
    pltpu.make_async_copy(gsend, grecv.at[me], recv_sems.at[GRAM]).start()
    with jax.named_scope("wait_gram"):
        arrive(GRAM, grecv)
    packed_ref[...] = jnp.sum(grecv[...], axis=0)

    most = pl.ds(0, half - 1)
    sent(ASK, recv1.at[most])
    sent(ASK_FAR, recv1_far)
    sent(TABLE, far_table)
    sent(SUM, recv2.at[0, most])
    sent(SUM_FAR, recv2.at[1, most])
    sent(BACK, recv3.at[0, most])
    sent(BACK_FAR, recv3.at[1])
    sent(GRAM, grecv.at[pl.ds(0, devices - 1)])


def finish(
    sizes,
    sketch_ref, packed_ref,
    sketch_hbm, basis_hbm, factor_hbm,
    basis_ref, factor_ref, sems,
):
    params, columns, height = sizes
    cam_width = sketch_ref.shape[1]
    sketch_copy = pltpu.make_async_copy(sketch_ref, sketch_hbm, sems.at[0])
    sketch_copy.start()
    with jax.named_scope("eliminate"):
        gram = unfold_gram(packed_ref[...], columns) / height
        strips = columns // STRIP
        unit = jnp.where(
            rows_iota((columns, columns)) == lanes_iota((columns, columns)), 1.0, 0.0
        )
        both = jnp.concatenate([unit, gram], axis=1)
        work = [both[s * STRIP : (s + 1) * STRIP] for s in range(strips)]
        row_ids = rows_iota((STRIP, 1))
        roots = [jnp.zeros((STRIP, LANES), F32) for _ in range(strips)]
        def spread_columns(first, least):
            low = columns + first * STRIP
            return [
                {
                    s: jnp.broadcast_to(work[s][:, low + j : low + j + 1], (STRIP, LANES))
                    for s in range(least, strips)
                }
                for j in range(STRIP)
            ]

        panel = spread_columns(0, 0)
        for base in range(strips):
            later = spread_columns(base + 1, base) if base + 1 < strips else []
            for j in range(0, STRIP, 2):
                a = panel[j][base][j : j + 1]
                b = panel[j + 1][base][j : j + 1]
                c = panel[j + 1][base][j + 1 : j + 2]
                det = a * c - b * b
                over_det, over_a = 1.0 / det, 1.0 / a
                roots[base] = jnp.where(row_ids == j, lax.rsqrt(a), roots[base])
                roots[base] = jnp.where(
                    row_ids == j + 1, lax.rsqrt(det * over_a), roots[base]
                )
                first, second, scale = {}, {}, {}
                for s in range(base, strips):
                    first[s] = panel[j][s] * c - panel[j + 1][s] * b
                    second[s] = panel[j + 1][s] * a - panel[j][s] * b
                    scale[s] = (
                        jnp.where(row_ids > j + 1, over_det, 0.0) if s == base else over_det
                    )
                for column in panel[j + 2 :] + later:
                    upper, lower = column[base][j : j + 1], column[base][j + 1 : j + 2]
                    for s in range(base, strips):
                        column[s] = column[s] - (first[s] * upper + second[s] * lower) * scale[s]
                upper, lower = work[base][j : j + 1], work[base][j + 1 : j + 2]
                beside = jnp.where(row_ids == j + 1, b * over_a, 0.0)[:, : 2 * columns]
                for s in range(base, strips):
                    step = (first[s] * scale[s])[:, : 2 * columns] * upper
                    step += (second[s] * scale[s])[:, : 2 * columns] * lower
                    if s == base:
                        step += beside * upper
                    work[s] = work[s] - step
            panel = later
        done = jnp.concatenate(
            [work[s] * roots[s][:, : 2 * columns] for s in range(strips)], axis=0
        )
        inverse = done[:, :columns]
        on_upper = rows_iota((columns, columns)) <= lanes_iota((columns, columns))
        factor_ref[...] = jnp.where(on_upper, done[:, columns:], 0.0)
    factor_copy = pltpu.make_async_copy(factor_ref, factor_hbm, sems.at[1])
    factor_copy.start()
    with jax.named_scope("basis"):
        flat = jnp.concatenate(
            [sketch_ref[row * columns : (row + 1) * columns] for row in range(params)], axis=1
        )
        basis = dot(inverse, flat, HIGH)
        for row in range(params):
            basis_ref[row * columns : (row + 1) * columns, :] = basis[
                :, row * cam_width : (row + 1) * cam_width
            ]
    basis_copy = pltpu.make_async_copy(basis_ref, basis_hbm, sems.at[2])
    basis_copy.start()
    with jax.named_scope("write"):
        sketch_copy.wait()
        factor_copy.wait()
        basis_copy.wait()


def on_device(omega, u_blocks, w_blocks, v_inverse, obs_camera, obs_track, obs_mask):
    track_count = lax.axis_size("track")
    cam_count = lax.axis_size("cam")
    devices = track_count * cam_count
    half = devices // 2
    columns, params, cam_width = omega.shape
    obs_count = obs_camera.shape[0]
    tracks = v_inverse.shape[2]
    capacity = max(2, 2 * obs_count // devices)
    rows = -(-capacity // (LANES // columns) // 8) * 8
    groups = -(-capacity // rows)
    span = half
    while span * rows * groups > CHUNK and span % 2 == 0:
        span //= 2
    chunk = span * rows * groups
    chunks = half // span

    table = omega.transpose(1, 0, 2).reshape(params * columns, cam_width)
    line = (1, obs_count)
    operands = (
        table,
        u_blocks,
        w_blocks,
        v_inverse,
        obs_camera.reshape(line),
        obs_track.reshape(line),
        obs_mask.reshape(line),
    )
    sizes = (track_count, cam_count, params, columns, rows, groups, span)
    message = pltpu.VMEM((2, half, 3 * rows, LANES), BF16)
    tall = columns * columns // 2 // LANES + 1
    wide_shape = (chunks, columns, chunk)
    pick_shape = (chunks, cam_width, chunk)
    whole = jax.ShapeDtypeStruct((params * columns, cam_width), F32)
    square = jax.ShapeDtypeStruct((columns, columns), F32)
    in_vmem = pl.BlockSpec(memory_space=pltpu.VMEM)
    anywhere = pl.BlockSpec(memory_space=pl.ANY)
    sketch, packed = pl.pallas_call(
        functools.partial(kernel, sizes),
        out_shape=(
            pltpu.VMEM((params * columns, cam_width), F32),
            pltpu.VMEM((tall, LANES), F32),
        ),
        in_specs=[anywhere] * 7,
        out_specs=(in_vmem,) * 2,
        scratch_shapes=[
            pltpu.VMEM((half, 2 * rows, LANES), BF16),
            pltpu.VMEM((half, 2 * rows, LANES), BF16),
            pltpu.VMEM((half, rows, LANES), BF16),
        ]
        + [message] * 4
        + [
            pltpu.VMEM((tall, LANES), F32),
            pltpu.VMEM((devices, tall, LANES), F32),
            pltpu.VMEM((params * columns, cam_width), BF16),
            pltpu.VMEM((columns, obs_count), F32),
            pltpu.VMEM((2, chunks, tracks, chunk), BF16),
            pltpu.VMEM((2,) + wide_shape, F32),
            pltpu.VMEM((2,) + pick_shape, BF16),
            pltpu.VMEM(wide_shape, F32),
            pltpu.VMEM(pick_shape, BF16),
            pltpu.VMEM((params * columns, cam_width), F32),
            pltpu.VMEM((params * columns, cam_width), F32),
            pltpu.VMEM((3 * columns, tracks), F32),
            pltpu.SemaphoreType.DMA((8,)),
            pltpu.SemaphoreType.DMA((8,)),
        ]
        + [pltpu.VMEM(array.shape, array.dtype) for array in operands]
        + [pltpu.SemaphoreType.DMA((len(operands),))],
        compiler_params=pltpu.CompilerParams(collective_id=0, has_side_effects=True),
    )(*operands)
    sketch, basis, factor = pl.pallas_call(
        functools.partial(finish, (params, columns, params * cam_width * devices)),
        out_shape=(whole, whole, square),
        in_specs=[in_vmem] * 2,
        out_specs=(anywhere,) * 3,
        scratch_shapes=[
            pltpu.VMEM((params * columns, cam_width), F32),
            pltpu.VMEM((columns, columns), F32),
            pltpu.SemaphoreType.DMA((3,)),
        ],
    )(*(pltpu.with_memory_space_constraint(x, pltpu.VMEM) for x in (sketch, packed)))

    def unfold(array):
        return array.reshape(params, columns, cam_width).transpose(1, 0, 2)

    return (unfold(sketch), unfold(basis), factor)


def solution(mesh):
    spread = P(None, None, ("track", "cam"))
    flat = P(("track", "cam"))
    return jax.shard_map(
        on_device,
        mesh=mesh,
        in_specs=(spread,) * 4 + (flat,) * 3,
        out_specs=(spread, spread, P()),
        check_vma=False,
    )
```

```python
import functools

import jax
import jax.numpy as jnp
from jax import lax
from jax.experimental import pallas as pl
from jax.experimental.pallas import tpu as pltpu
from jax.sharding import PartitionSpec as P

BLK_OBS = 128
TRK_BLK = 32
LANES = 128
STRIP = 8
CHUNK = 512
UNROLL = 32

LOGICAL = pl.DeviceIdType.LOGICAL
NT = (((1,), (1,)), ((), ()))
F32 = jnp.float32
BF16 = jnp.bfloat16

ASK, ASK_FAR, TABLE, SUM, SUM_FAR, BACK, BACK_FAR, GRAM = range(8)


def dot(left, right, precision=None):
    return jnp.dot(left, right, precision=precision, preferred_element_type=F32)


def dot_nt(left, right, precision=None):
    return lax.dot_general(left, right, NT, precision=precision, preferred_element_type=F32)


def one_hot(condition):
    return jnp.where(condition, 1.0, 0.0).astype(BF16)


def rows_iota(shape):
    return lax.broadcasted_iota(jnp.int32, shape, 0)


def lanes_iota(shape):
    return lax.broadcasted_iota(jnp.int32, shape, 1)


def turns(first, count, body):
    if count - first <= UNROLL:
        for turn in range(first, count):
            body(turn)
    else:
        pl.loop(first, count)(body)


def repeat(count, body):
    if count == 1:
        body(0)
    else:
        pl.loop(0, count)(body)


def fold(gram):
    columns = gram.shape[0]
    middle = columns // 2
    folds = LANES // columns
    tall = middle // folds
    top, bottom = gram[:middle], gram[middle:]
    first, second = [], []
    for k in range(folds):
        first.append(top[k * tall : (k + 1) * tall])
        piece = bottom[k * tall : (k + 1) * tall]
        second += [piece[:, middle:], piece[:, :middle]]
    lane = lanes_iota((tall, LANES))
    row = rows_iota((tall, LANES)) + lane // columns * tall
    packed = jnp.where(
        lax.rem(lane, columns) >= row,
        jnp.concatenate(first, axis=1),
        jnp.concatenate(second, axis=1),
    )
    shape = (middle, columns)
    on_diagonal = lanes_iota(shape) == rows_iota(shape) + middle
    diagonal = jnp.sum(jnp.where(on_diagonal, bottom, 0.0), axis=0, keepdims=True)
    diagonal = jnp.concatenate([diagonal, jnp.zeros((1, LANES - columns), F32)], axis=1)
    return jnp.concatenate([packed, diagonal], axis=0)


def unfold_gram(packed, columns):
    middle = columns // 2
    folds = LANES // columns
    tall = middle // folds
    both = jnp.concatenate(
        [packed[:tall, k * columns : (k + 1) * columns] for k in range(folds)], axis=0
    )
    gap = jnp.zeros((tall, middle), F32)
    moved = jnp.concatenate(
        [
            jnp.concatenate([gap, packed[:tall, k * columns : k * columns + middle]], axis=1)
            for k in range(folds)
        ],
        axis=0,
    )
    shape = (middle, columns)
    row, lane = rows_iota(shape), lanes_iota(shape)
    top = jnp.where(lane >= row, both, 0.0)
    bottom = jnp.where(lane < row + middle, moved, 0.0)
    bottom += jnp.where(lane == row + middle, packed[tall : tall + 1, :columns], 0.0)
    half = jnp.concatenate([top, bottom], axis=0)
    square = (columns, columns)
    wide = jnp.concatenate([half, jnp.zeros((columns, LANES - columns), F32)], axis=1)
    turned = jnp.concatenate([wide] + [jnp.zeros((LANES - columns, LANES), F32)], axis=0).T
    turned = turned[:columns, :columns]
    return half + jnp.where(lanes_iota(square) == rows_iota(square), 0.0, turned)


def kernel(
    sizes,
    omega_hbm, u_hbm, w_hbm, v_hbm, camera_hbm, track_hbm, mask_hbm,
    sketch_ref, packed_ref,
    send1, recv1, recv1_far, send2, recv2, send3, recv3, gsend, grecv, far_table,
    fields, to_track, wide, pick, far_wide, far_pick, own, sum_ref,
    send_sems, recv_sems,
    omega_ref, u_ref, w_ref, v_ref, camera_ref, track_ref, mask_ref, load_sems,
):
    track_count, cam_count, params, columns, rows, groups, span = sizes
    devices = track_count * cam_count
    half = devices // 2
    cam_width = omega_ref.shape[1]
    obs_count = camera_ref.shape[1]
    tracks = v_ref.shape[2]
    part_rows = span * rows
    chunk = groups * part_rows
    chunks = half // span
    me = lax.axis_index("track") * cam_count + lax.axis_index("cam")
    side = me // half
    place_at = me - side * half
    home = side * half
    away = half - home

    def wrapped(start, turn, count):
        place = start + turn
        return jnp.where(place >= count, place - count, place)

    barrier = pltpu.get_barrier_semaphore()

    def greet(device):
        pl.semaphore_signal(barrier, inc=1, device_id=device, device_id_type=LOGICAL)

    turns(1, half, lambda turn: greet(home + wrapped(place_at, turn, half)))
    greet(away + place_at)

    loads = [
        pltpu.make_async_copy(source, target, load_sems.at[index])
        for index, (source, target) in enumerate(
            [
                (camera_hbm, camera_ref),
                (track_hbm, track_ref),
                (mask_hbm, mask_ref),
                (w_hbm, w_ref),
                (omega_hbm, omega_ref),
                (u_hbm, u_ref),
                (v_hbm, v_ref),
            ]
        )
    ]
    for load in loads:
        load.start()

    def remote(index, src, dst, device):
        return pltpu.make_async_remote_copy(
            src_ref=src,
            dst_ref=dst,
            send_sem=send_sems.at[index],
            recv_sem=recv_sems.at[index],
            device_id=device,
            device_id_type=LOGICAL,
        )

    def to_home(index, src, dst):
        def send(turn):
            other = wrapped(place_at, turn, half)
            remote(index, src.at[other], dst.at[place_at], home + other).start()

        turns(1, half, send)
        pltpu.make_async_copy(src.at[place_at], dst.at[place_at], recv_sems.at[index]).start()

    near_first = lax.rem(place_at, half // 2) + side * (half // 2)

    def to_away(index, src, dst):
        def send(turn):
            other = wrapped(near_first, turn, half)
            remote(index, src(other), dst.at[place_at], away + other).start()

        turns(0, half, send)

    def arrive(index, dst):
        pltpu.make_async_copy(dst, dst, recv_sems.at[index]).wait()

    def sent(index, part):
        pltpu.make_async_copy(part, part, send_sems.at[index]).wait()

    def pack(part, values, dst, at=0):
        for index in range(values.shape[0] // columns):
            block = values[index * columns : (index + 1) * columns]
            pieces = [block[:, g * part_rows : (g + 1) * part_rows] for g in range(groups)]
            if groups * columns < LANES:
                pieces.append(jnp.zeros((LANES - groups * columns, part_rows), F32))
            turned = jnp.concatenate(pieces, axis=0).T.reshape(span, rows, LANES)
            low = at + index * rows
            dst[pl.ds(part * span, span), low : low + rows] = turned.astype(BF16)

    def unpack(part, src, at, count):
        blocks = []
        for index in range(count):
            low = at + index * rows
            block = src[pl.ds(part * span, span), low : low + rows]
            turned = block.reshape(part_rows, LANES).astype(F32).T
            blocks.append(
                jnp.concatenate(
                    [turned[g * columns : (g + 1) * columns] for g in range(groups)], axis=1
                )
            )
        return jnp.concatenate(blocks, axis=0)

    with jax.named_scope("place"):
        for load in loads[:4]:
            load.wait()
        camera = camera_ref[...]
        owner = camera // cam_width
        local = camera - owner * cam_width
        owner = owner - home
        owner = jnp.where(owner < 0, owner + devices, owner)
        track_id = lanes_iota((1, obs_count)) // BLK_OBS * TRK_BLK + track_ref[...]
        live = mask_ref[...].astype(F32)
        fields[...] = jnp.zeros_like(fields)
        for row in range(params):
            fields[3 * row : 3 * row + 3, :] = w_ref[row].astype(F32) * live
        high = local // 256
        fields[3 * params : 3 * params + 1, :] = high.astype(F32)
        fields[3 * params + 1 : 3 * params + 2, :] = (local - high * 256).astype(F32)
        owned = one_hot(rows_iota((devices, obs_count)) == owner)
        earlier = one_hot(rows_iota((obs_count, obs_count)) < lanes_iota((obs_count, obs_count)))
        ranks = dot(owned, earlier)
        rank = jnp.sum(ranks * owned.astype(F32), axis=0, keepdims=True).astype(jnp.int32)
        group = jnp.zeros_like(rank)
        for g in range(1, groups):
            group += jnp.where(rank >= g * rows, 1, 0)
        offset = group * part_rows + rank - group * rows
        member = one_hot(rows_iota((tracks, obs_count)) == track_id)
        table = jnp.concatenate([fields[...].astype(BF16), member], axis=0)

        for far in range(2):

            def place(part):
                nearby = owner - far * half - part * span
                inside = jnp.logical_and(nearby >= 0, nearby < span)
                slot = jnp.where(inside, nearby * rows + offset, -1)
                slots = one_hot(rows_iota((chunk, obs_count)) == slot)
                placed = dot_nt(table, slots)
                pack(part, placed[:columns], send1, far * rows)
                to_track[far, part] = placed[columns:].astype(BF16)

            repeat(chunks, place)

    with jax.named_scope("barrier"):
        loads[4].wait()
        pl.semaphore_wait(barrier, half)
    table_copy = remote(TABLE, omega_ref, far_table, away + place_at)
    to_home(ASK, send1, recv1)
    table_copy.start()

    with jax.named_scope("own"):
        for load in loads[5:]:
            load.wait()
        for row in range(params):
            total = jnp.zeros((columns, cam_width), F32)
            for col in range(params):
                total += u_ref[row, col : col + 1, :] * omega_ref[
                    col * columns : (col + 1) * columns, :
                ].astype(F32)
            own[row * columns : (row + 1) * columns, :] = total
        sum_ref[...] = jnp.zeros_like(sum_ref)

    def read_request(part, src, at, wide_to, pick_to):
        turned = unpack(part, src, at, 1)
        wide_to[part] = turned
        number = turned[3 * params : 3 * params + 1] * 256.0 + turned[
            3 * params + 1 : 3 * params + 2
        ]
        pick_to[part] = one_hot(rows_iota((cam_width, chunk)) == number.astype(jnp.int32))

    def project(part, cameras, weights, chosen, dst):
        gathered = dot(cameras[...], chosen[part])
        turned = weights[part]
        pieces = []
        for comp in range(3):
            total = jnp.zeros((columns, chunk), F32)
            for row in range(params):
                at = row * 3 + comp
                total += turned[at : at + 1] * gathered[row * columns : (row + 1) * columns]
            pieces.append(total)
        pack(part, jnp.concatenate(pieces, axis=0), dst)

    with jax.named_scope("wait_ask"):
        arrive(ASK, recv1)
    with jax.named_scope("project"):
        repeat(chunks, lambda part: read_request(part, recv1, 0, wide.at[0], pick.at[0]))
        repeat(chunks, lambda part: read_request(part, recv1, rows, far_wide, far_pick))
        repeat(chunks, lambda part: project(part, omega_ref, wide.at[0], pick.at[0], send2.at[0]))
    to_home(SUM, send2.at[0], recv2.at[0])
    with jax.named_scope("wait_table"):
        arrive(TABLE, far_table)
    with jax.named_scope("project_far"):
        repeat(chunks, lambda part: project(part, far_table, far_wide, far_pick, send2.at[1]))
    to_home(SUM_FAR, send2.at[1], recv2.at[1])
    to_away(ASK_FAR, lambda other: send1.at[other, pl.ds(rows, rows)], recv1_far)

    def collect(far, part):
        values = unpack(part, recv2.at[far], 0, 3).astype(BF16)
        sum_ref[...] += dot_nt(values, to_track[far, part])

    with jax.named_scope("wait_sum"):
        arrive(SUM, recv2.at[0])
    with jax.named_scope("collect"):
        repeat(chunks, lambda part: collect(0, part))
    with jax.named_scope("wait_sum_far"):
        arrive(SUM_FAR, recv2.at[1])
    with jax.named_scope("collect_far"):
        repeat(chunks, lambda part: collect(1, part))
        pieces = []
        for row in range(3):
            total = jnp.zeros((columns, tracks), F32)
            for col in range(3):
                total += v_ref[row, col : col + 1, :] * sum_ref[
                    col * columns : (col + 1) * columns
                ]
            pieces.append(total)
        solved = jnp.concatenate(pieces, axis=0).astype(BF16)
        repeat(
            chunks, lambda part: pack(part, dot(solved, to_track[1, part]), send3.at[1])
        )
    to_away(BACK_FAR, lambda other: send3.at[1, other], recv3.at[1])
    with jax.named_scope("spread"):
        repeat(
            chunks, lambda part: pack(part, dot(solved, to_track[0, part]), send3.at[0])
        )
    to_home(BACK, send3.at[0], recv3.at[0])
    with jax.named_scope("read_ask_far"):
        arrive(ASK_FAR, recv1_far)
        repeat(chunks, lambda part: read_request(part, recv1_far, 0, wide.at[1], pick.at[1]))

    def gather_back(far, part):
        turned = unpack(part, recv3.at[far], 0, 3)
        weights = wide[far, part]
        pieces = []
        for row in range(params):
            total = jnp.zeros((columns, chunk), F32)
            for comp in range(3):
                at = row * 3 + comp
                total += weights[at : at + 1] * turned[comp * columns : (comp + 1) * columns]
            pieces.append(total)
        contribution = jnp.concatenate(pieces, axis=0).astype(BF16)
        own[...] -= dot_nt(contribution, pick[far, part])

    with jax.named_scope("wait_back"):
        arrive(BACK, recv3.at[0])
    with jax.named_scope("gather"):
        repeat(chunks, lambda part: gather_back(0, part))
    with jax.named_scope("wait_back_far"):
        arrive(BACK_FAR, recv3.at[1])
    with jax.named_scope("gather_far"):
        repeat(chunks, lambda part: gather_back(1, part))

        sketch = own[...]
        sketch_ref[...] = sketch
        flat = jnp.concatenate(
            [sketch[row * columns : (row + 1) * columns] for row in range(params)], axis=1
        )
        head = flat.astype(BF16)
        rest = (flat - head.astype(F32)).astype(BF16)
        parts = jnp.concatenate([head, rest], axis=0)
        products = dot_nt(parts, parts)
        products = products[:columns] + products[columns:]
        gsend[...] = fold(products[:, :columns]) + fold(products[:, columns:])

    def send_gram(turn):
        remote(GRAM, gsend, grecv.at[me], wrapped(me, turn, devices)).start()

    turns(1, devices, send_gram)
    pltpu.make_async_copy(gsend, grecv.at[me], recv_sems.at[GRAM]).start()
    most = pl.ds(0, half - 1)
    sent(ASK, recv1.at[most])
    sent(ASK_FAR, recv1_far)
    sent(TABLE, far_table)
    sent(SUM, recv2.at[0, most])
    sent(SUM_FAR, recv2.at[1, most])
    sent(BACK, recv3.at[0, most])
    sent(BACK_FAR, recv3.at[1])
    with jax.named_scope("wait_gram"):
        arrive(GRAM, grecv)
    packed_ref[...] = jnp.sum(grecv[...], axis=0)

    sent(GRAM, grecv.at[pl.ds(0, devices - 1)])


def finish(
    sizes,
    sketch_ref, packed_ref,
    sketch_hbm, basis_hbm, factor_hbm,
    basis_ref, factor_ref, sems,
):
    params, columns, height = sizes
    cam_width = sketch_ref.shape[1]
    sketch_copy = pltpu.make_async_copy(sketch_ref, sketch_hbm, sems.at[0])
    sketch_copy.start()
    with jax.named_scope("eliminate"):
        gram = unfold_gram(packed_ref[...], columns) / height
        strips = columns // STRIP
        unit = jnp.where(
            rows_iota((columns, columns)) == lanes_iota((columns, columns)), 1.0, 0.0
        )
        both = jnp.concatenate([unit, gram, unit, unit], axis=1)
        work = [both[s * STRIP : (s + 1) * STRIP] for s in range(strips)]
        row_ids = rows_iota((STRIP, 1))
        roots = [jnp.zeros((STRIP, LANES), F32) for _ in range(strips)]
        def spread_columns(first, least):
            low = columns + first * STRIP
            return [
                {
                    s: jnp.broadcast_to(work[s][:, low + j : low + j + 1], (STRIP, LANES))
                    for s in range(least, strips)
                }
                for j in range(STRIP)
            ]

        panel = spread_columns(0, 0)
        for base in range(strips):
            later = spread_columns(base + 1, base) if base + 1 < strips else []
            for j in range(0, STRIP, 2):
                a = panel[j][base][j : j + 1]
                b = panel[j + 1][base][j : j + 1]
                c = panel[j + 1][base][j + 1 : j + 2]
                det = a * c - b * b
                over_det, over_a = 1.0 / det, 1.0 / a
                roots[base] = jnp.where(row_ids == j, lax.rsqrt(a), roots[base])
                roots[base] = jnp.where(
                    row_ids == j + 1, lax.rsqrt(det * over_a), roots[base]
                )
                first, second, scale = {}, {}, {}
                for s in range(base, strips):
                    first[s] = panel[j][s] * c - panel[j + 1][s] * b
                    second[s] = panel[j + 1][s] * a - panel[j][s] * b
                    scale[s] = (
                        jnp.where(row_ids > j + 1, over_det, 0.0) if s == base else over_det
                    )
                for column in panel[j + 2 :] + later:
                    upper, lower = column[base][j : j + 1], column[base][j + 1 : j + 2]
                    for s in range(base, strips):
                        column[s] = column[s] - (first[s] * upper + second[s] * lower) * scale[s]
                upper, lower = work[base][j : j + 1], work[base][j + 1 : j + 2]
                beside = jnp.where(row_ids == j + 1, b * over_a, 0.0)
                for s in range(base, strips):
                    step = (first[s] * scale[s]) * upper
                    step += (second[s] * scale[s]) * lower
                    if s == base:
                        step += beside * upper
                    work[s] = work[s] - step
            panel = later
        done = jnp.concatenate(
            [work[s] * roots[s] for s in range(strips)], axis=0
        )
        on_upper = rows_iota((columns, columns)) <= lanes_iota((columns, columns))
        factor_ref[...] = jnp.where(on_upper, done[:, columns : 2 * columns], 0.0)
    factor_copy = pltpu.make_async_copy(factor_ref, factor_hbm, sems.at[1])
    factor_copy.start()
    with jax.named_scope("basis"):
        flat = jnp.concatenate(
            [sketch_ref[row * columns : (row + 1) * columns] for row in range(params)], axis=1
        )
        head = flat.astype(BF16)
        rest = (flat - head.astype(F32)).astype(BF16)
        upper = done.astype(BF16)
        lower = (done - upper.astype(F32)).astype(BF16)
        left = jnp.where(lanes_iota(done.shape) < 3 * columns, upper, lower)
        right = jnp.concatenate([head, jnp.zeros_like(head), rest, head], axis=0)
        basis = dot(left, right)
        for row in range(params):
            basis_ref[row * columns : (row + 1) * columns, :] = basis[
                :, row * cam_width : (row + 1) * cam_width
            ]
    basis_copy = pltpu.make_async_copy(basis_ref, basis_hbm, sems.at[2])
    basis_copy.start()
    with jax.named_scope("write"):
        sketch_copy.wait()
        factor_copy.wait()
        basis_copy.wait()


def on_device(omega, u_blocks, w_blocks, v_inverse, obs_camera, obs_track, obs_mask):
    track_count = lax.axis_size("track")
    cam_count = lax.axis_size("cam")
    devices = track_count * cam_count
    half = devices // 2
    columns, params, cam_width = omega.shape
    obs_count = obs_camera.shape[0]
    tracks = v_inverse.shape[2]
    capacity = max(2, 2 * obs_count // devices)
    rows = -(-capacity // (LANES // columns) // 8) * 8
    groups = -(-capacity // rows)
    span = half
    while span * rows * groups > CHUNK and span % 2 == 0:
        span //= 2
    chunk = span * rows * groups
    chunks = half // span

    table = omega.transpose(1, 0, 2).reshape(params * columns, cam_width)
    line = (1, obs_count)
    operands = (
        table,
        u_blocks,
        w_blocks,
        v_inverse,
        obs_camera.reshape(line),
        obs_track.reshape(line),
        obs_mask.reshape(line),
    )
    sizes = (track_count, cam_count, params, columns, rows, groups, span)
    message = pltpu.VMEM((2, half, 3 * rows, LANES), BF16)
    tall = columns * columns // 2 // LANES + 1
    wide_shape = (chunks, columns, chunk)
    pick_shape = (chunks, cam_width, chunk)
    whole = jax.ShapeDtypeStruct((params * columns, cam_width), F32)
    square = jax.ShapeDtypeStruct((columns, columns), F32)
    in_vmem = pl.BlockSpec(memory_space=pltpu.VMEM)
    anywhere = pl.BlockSpec(memory_space=pl.ANY)
    sketch, packed = pl.pallas_call(
        functools.partial(kernel, sizes),
        out_shape=(
            pltpu.VMEM((params * columns, cam_width), F32),
            pltpu.VMEM((tall, LANES), F32),
        ),
        in_specs=[anywhere] * 7,
        out_specs=(in_vmem,) * 2,
        scratch_shapes=[
            pltpu.VMEM((half, 2 * rows, LANES), BF16),
            pltpu.VMEM((half, 2 * rows, LANES), BF16),
            pltpu.VMEM((half, rows, LANES), BF16),
        ]
        + [message] * 4
        + [
            pltpu.VMEM((tall, LANES), F32),
            pltpu.VMEM((devices, tall, LANES), F32),
            pltpu.VMEM((params * columns, cam_width), BF16),
            pltpu.VMEM((columns, obs_count), F32),
            pltpu.VMEM((2, chunks, tracks, chunk), BF16),
            pltpu.VMEM((2,) + wide_shape, F32),
            pltpu.VMEM((2,) + pick_shape, BF16),
            pltpu.VMEM(wide_shape, F32),
            pltpu.VMEM(pick_shape, BF16),
            pltpu.VMEM((params * columns, cam_width), F32),
            pltpu.VMEM((3 * columns, tracks), F32),
            pltpu.SemaphoreType.DMA((8,)),
            pltpu.SemaphoreType.DMA((8,)),
        ]
        + [pltpu.VMEM(array.shape, array.dtype) for array in operands]
        + [pltpu.SemaphoreType.DMA((len(operands),))],
        compiler_params=pltpu.CompilerParams(collective_id=0, has_side_effects=True),
    )(*operands)
    sketch, basis, factor = pl.pallas_call(
        functools.partial(finish, (params, columns, params * cam_width * devices)),
        out_shape=(whole, whole, square),
        in_specs=[in_vmem] * 2,
        out_specs=(anywhere,) * 3,
        scratch_shapes=[
            pltpu.VMEM((params * columns, cam_width), F32),
            pltpu.VMEM((columns, columns), F32),
            pltpu.SemaphoreType.DMA((3,)),
        ],
    )(*(pltpu.with_memory_space_constraint(x, pltpu.VMEM) for x in (sketch, packed)))

    def unfold(array):
        return array.reshape(params, columns, cam_width).transpose(1, 0, 2)

    return (unfold(sketch), unfold(basis), factor)


def solution(mesh):
    spread = P(None, None, ("track", "cam"))
    flat = P(("track", "cam"))
    return jax.shard_map(
        on_device,
        mesh=mesh,
        in_specs=(spread,) * 4 + (flat,) * 3,
        out_specs=(spread, spread, P()),
        check_vma=False,
    )
```

```python
import functools

import jax
import jax.numpy as jnp
from jax import lax
from jax.experimental import pallas as pl
from jax.experimental.pallas import tpu as pltpu
from jax.sharding import PartitionSpec as P

BLK_OBS = 128
TRK_BLK = 32
LANES = 128
STRIP = 8
CHUNK = 512
UNROLL = 32

LOGICAL = pl.DeviceIdType.LOGICAL
NT = (((1,), (1,)), ((), ()))
F32 = jnp.float32
BF16 = jnp.bfloat16

ASK, ASK_FAR, TABLE, SUM, SUM_FAR, BACK, BACK_FAR, GRAM = range(8)


def dot(left, right, precision=None):
    return jnp.dot(left, right, precision=precision, preferred_element_type=F32)


def dot_nt(left, right, precision=None):
    return lax.dot_general(left, right, NT, precision=precision, preferred_element_type=F32)


def one_hot(condition):
    return jnp.where(condition, 1.0, 0.0).astype(BF16)


def rows_iota(shape):
    return lax.broadcasted_iota(jnp.int32, shape, 0)


def lanes_iota(shape):
    return lax.broadcasted_iota(jnp.int32, shape, 1)


def turns(first, count, body):
    if count - first <= UNROLL:
        for turn in range(first, count):
            body(turn)
    else:
        pl.loop(first, count)(body)


def repeat(count, body):
    if count == 1:
        body(0)
    else:
        pl.loop(0, count)(body)


def fold(gram):
    columns = gram.shape[0]
    middle = columns // 2
    folds = LANES // columns
    tall = middle // folds
    top, bottom = gram[:middle], gram[middle:]
    first, second = [], []
    for k in range(folds):
        first.append(top[k * tall : (k + 1) * tall])
        piece = bottom[k * tall : (k + 1) * tall]
        second += [piece[:, middle:], piece[:, :middle]]
    lane = lanes_iota((tall, LANES))
    row = rows_iota((tall, LANES)) + lane // columns * tall
    packed = jnp.where(
        lax.rem(lane, columns) >= row,
        jnp.concatenate(first, axis=1),
        jnp.concatenate(second, axis=1),
    )
    shape = (middle, columns)
    on_diagonal = lanes_iota(shape) == rows_iota(shape) + middle
    diagonal = jnp.sum(jnp.where(on_diagonal, bottom, 0.0), axis=0, keepdims=True)
    diagonal = jnp.concatenate([diagonal, jnp.zeros((1, LANES - columns), F32)], axis=1)
    return jnp.concatenate([packed, diagonal], axis=0)


def unfold_gram(packed, columns):
    middle = columns // 2
    folds = LANES // columns
    tall = middle // folds
    both = jnp.concatenate(
        [packed[:tall, k * columns : (k + 1) * columns] for k in range(folds)], axis=0
    )
    gap = jnp.zeros((tall, middle), F32)
    moved = jnp.concatenate(
        [
            jnp.concatenate([gap, packed[:tall, k * columns : k * columns + middle]], axis=1)
            for k in range(folds)
        ],
        axis=0,
    )
    shape = (middle, columns)
    row, lane = rows_iota(shape), lanes_iota(shape)
    top = jnp.where(lane >= row, both, 0.0)
    bottom = jnp.where(lane < row + middle, moved, 0.0)
    bottom += jnp.where(lane == row + middle, packed[tall : tall + 1, :columns], 0.0)
    half = jnp.concatenate([top, bottom], axis=0)
    square = (columns, columns)
    wide = jnp.concatenate([half, jnp.zeros((columns, LANES - columns), F32)], axis=1)
    turned = jnp.concatenate([wide] + [jnp.zeros((LANES - columns, LANES), F32)], axis=0).T
    turned = turned[:columns, :columns]
    return half + jnp.where(lanes_iota(square) == rows_iota(square), 0.0, turned)


def kernel(
    sizes,
    omega_hbm, u_hbm, w_hbm, v_hbm, camera_hbm, track_hbm, mask_hbm,
    sketch_ref, packed_ref,
    send1, recv1, recv1_far, send2, recv2, send3, recv3, gsend, grecv, far_table,
    fields, to_track, wide, pick, far_wide, far_pick, own, sum_ref,
    send_sems, recv_sems,
    omega_ref, u_ref, w_ref, v_ref, camera_ref, track_ref, mask_ref, load_sems,
):
    track_count, cam_count, params, columns, rows, groups, span = sizes
    devices = track_count * cam_count
    half = devices // 2
    cam_width = omega_ref.shape[1]
    obs_count = camera_ref.shape[1]
    tracks = v_ref.shape[2]
    part_rows = span * rows
    chunk = groups * part_rows
    chunks = half // span
    me = lax.axis_index("track") * cam_count + lax.axis_index("cam")
    side = me // half
    place_at = me - side * half
    home = side * half
    away = half - home

    def wrapped(start, turn, count):
        place = start + turn
        return jnp.where(place >= count, place - count, place)

    barrier = pltpu.get_barrier_semaphore()

    def greet(device):
        pl.semaphore_signal(barrier, inc=1, device_id=device, device_id_type=LOGICAL)

    turns(1, half, lambda turn: greet(home + wrapped(place_at, turn, half)))
    greet(away + place_at)

    loads = [
        pltpu.make_async_copy(source, target, load_sems.at[index])
        for index, (source, target) in enumerate(
            [
                (camera_hbm, camera_ref),
                (track_hbm, track_ref),
                (mask_hbm, mask_ref),
                (w_hbm, w_ref),
                (omega_hbm, omega_ref),
                (u_hbm, u_ref),
                (v_hbm, v_ref),
            ]
        )
    ]
    for load in loads:
        load.start()

    def remote(index, src, dst, device):
        return pltpu.make_async_remote_copy(
            src_ref=src,
            dst_ref=dst,
            send_sem=send_sems.at[index],
            recv_sem=recv_sems.at[index],
            device_id=device,
            device_id_type=LOGICAL,
        )

    def to_home(index, src, dst):
        def send(turn):
            other = wrapped(place_at, turn, half)
            remote(index, src.at[other], dst.at[place_at], home + other).start()

        turns(1, half, send)
        pltpu.make_async_copy(src.at[place_at], dst.at[place_at], recv_sems.at[index]).start()

    quarter = half // 2 if half % 2 == 0 else half
    in_quarter = lax.rem(place_at, quarter)

    def far_place(turn):
        other = wrapped(in_quarter, turn % quarter, quarter)
        if quarter == half:
            return other
        return other + quarter * (1 - side + (2 * side - 1) * (turn // quarter))

    def to_away(index, src, dst):
        def send(turn):
            other = far_place(turn)
            remote(index, src(other), dst.at[place_at], away + other).start()

        turns(0, half, send)

    def arrive(index, dst):
        pltpu.make_async_copy(dst, dst, recv_sems.at[index]).wait()

    def sent(index, part):
        pltpu.make_async_copy(part, part, send_sems.at[index]).wait()

    def pack(part, values, dst, at=0):
        for index in range(values.shape[0] // columns):
            block = values[index * columns : (index + 1) * columns]
            pieces = [block[:, g * part_rows : (g + 1) * part_rows] for g in range(groups)]
            if groups * columns < LANES:
                pieces.append(jnp.zeros((LANES - groups * columns, part_rows), F32))
            turned = jnp.concatenate(pieces, axis=0).T.reshape(span, rows, LANES)
            low = at + index * rows
            dst[pl.ds(part * span, span), low : low + rows] = turned.astype(BF16)

    def unpack(part, src, at, count):
        blocks = []
        for index in range(count):
            low = at + index * rows
            block = src[pl.ds(part * span, span), low : low + rows]
            turned = block.reshape(part_rows, LANES).astype(F32).T
            blocks.append(
                jnp.concatenate(
                    [turned[g * columns : (g + 1) * columns] for g in range(groups)], axis=1
                )
            )
        return jnp.concatenate(blocks, axis=0)

    with jax.named_scope("place"):
        for load in loads[:4]:
            load.wait()
        camera = camera_ref[...]
        owner = camera // cam_width
        local = camera - owner * cam_width
        owner = owner - home
        owner = jnp.where(owner < 0, owner + devices, owner)
        track_id = lanes_iota((1, obs_count)) // BLK_OBS * TRK_BLK + track_ref[...]
        live = mask_ref[...].astype(F32)
        fields[...] = jnp.zeros_like(fields)
        for row in range(params):
            fields[3 * row : 3 * row + 3, :] = w_ref[row].astype(F32) * live
        high = local // 256
        fields[3 * params : 3 * params + 1, :] = high.astype(F32)
        fields[3 * params + 1 : 3 * params + 2, :] = (local - high * 256).astype(F32)
        owned = one_hot(rows_iota((devices, obs_count)) == owner)
        earlier = one_hot(rows_iota((obs_count, obs_count)) < lanes_iota((obs_count, obs_count)))
        ranks = dot(owned, earlier)
        rank = jnp.sum(ranks * owned.astype(F32), axis=0, keepdims=True).astype(jnp.int32)
        group = jnp.zeros_like(rank)
        for g in range(1, groups):
            group += jnp.where(rank >= g * rows, 1, 0)
        offset = group * part_rows + rank - group * rows
        member = one_hot(rows_iota((tracks, obs_count)) == track_id)
        table = jnp.concatenate([fields[...].astype(BF16), member], axis=0)

        for far in range(2):

            def place(part):
                nearby = owner - far * half - part * span
                inside = jnp.logical_and(nearby >= 0, nearby < span)
                slot = jnp.where(inside, nearby * rows + offset, -1)
                slots = one_hot(rows_iota((chunk, obs_count)) == slot)
                placed = dot_nt(table, slots)
                pack(part, placed[:columns], send1, far * rows)
                to_track[far, part] = placed[columns:].astype(BF16)

            repeat(chunks, place)

    with jax.named_scope("barrier"):
        loads[4].wait()
        pl.semaphore_wait(barrier, half)
    table_copy = remote(TABLE, omega_ref, far_table, away + place_at)
    to_home(ASK, send1, recv1)
    table_copy.start()

    with jax.named_scope("own"):
        for load in loads[5:]:
            load.wait()
        for row in range(params):
            total = jnp.zeros((columns, cam_width), F32)
            for col in range(params):
                total += u_ref[row, col : col + 1, :] * omega_ref[
                    col * columns : (col + 1) * columns, :
                ].astype(F32)
            own[row * columns : (row + 1) * columns, :] = total
        sum_ref[...] = jnp.zeros_like(sum_ref)

    def read_request(part, src, at, wide_to, pick_to):
        turned = unpack(part, src, at, 1)
        wide_to[part] = turned
        number = turned[3 * params : 3 * params + 1] * 256.0 + turned[
            3 * params + 1 : 3 * params + 2
        ]
        pick_to[part] = one_hot(rows_iota((cam_width, chunk)) == number.astype(jnp.int32))

    def project(part, cameras, weights, chosen, dst):
        gathered = dot(cameras[...], chosen[part])
        turned = weights[part]
        pieces = []
        for comp in range(3):
            total = jnp.zeros((columns, chunk), F32)
            for row in range(params):
                at = row * 3 + comp
                total += turned[at : at + 1] * gathered[row * columns : (row + 1) * columns]
            pieces.append(total)
        pack(part, jnp.concatenate(pieces, axis=0), dst)

    with jax.named_scope("wait_ask"):
        arrive(ASK, recv1)
    with jax.named_scope("project"):
        repeat(chunks, lambda part: read_request(part, recv1, 0, wide.at[0], pick.at[0]))
        repeat(chunks, lambda part: read_request(part, recv1, rows, far_wide, far_pick))
        repeat(chunks, lambda part: project(part, omega_ref, wide.at[0], pick.at[0], send2.at[0]))
    to_home(SUM, send2.at[0], recv2.at[0])
    with jax.named_scope("wait_table"):
        arrive(TABLE, far_table)
    with jax.named_scope("project_far"):
        repeat(chunks, lambda part: project(part, far_table, far_wide, far_pick, send2.at[1]))
    to_home(SUM_FAR, send2.at[1], recv2.at[1])
    to_away(ASK_FAR, lambda other: send1.at[other, pl.ds(rows, rows)], recv1_far)

    def collect(far, part):
        values = unpack(part, recv2.at[far], 0, 3).astype(BF16)
        sum_ref[...] += dot_nt(values, to_track[far, part])

    with jax.named_scope("wait_sum"):
        arrive(SUM, recv2.at[0])
    with jax.named_scope("collect"):
        repeat(chunks, lambda part: collect(0, part))
    with jax.named_scope("wait_sum_far"):
        arrive(SUM_FAR, recv2.at[1])
    with jax.named_scope("collect_far"):
        repeat(chunks, lambda part: collect(1, part))
        pieces = []
        for row in range(3):
            total = jnp.zeros((columns, tracks), F32)
            for col in range(3):
                total += v_ref[row, col : col + 1, :] * sum_ref[
                    col * columns : (col + 1) * columns
                ]
            pieces.append(total)
        solved = jnp.concatenate(pieces, axis=0).astype(BF16)
        repeat(
            chunks, lambda part: pack(part, dot(solved, to_track[1, part]), send3.at[1])
        )
    to_away(BACK_FAR, lambda other: send3.at[1, other], recv3.at[1])
    with jax.named_scope("spread"):
        repeat(
            chunks, lambda part: pack(part, dot(solved, to_track[0, part]), send3.at[0])
        )
    to_home(BACK, send3.at[0], recv3.at[0])
    with jax.named_scope("read_ask_far"):
        arrive(ASK_FAR, recv1_far)
        repeat(chunks, lambda part: read_request(part, recv1_far, 0, wide.at[1], pick.at[1]))

    def gather_back(far, part):
        turned = unpack(part, recv3.at[far], 0, 3)
        weights = wide[far, part]
        pieces = []
        for row in range(params):
            total = jnp.zeros((columns, chunk), F32)
            for comp in range(3):
                at = row * 3 + comp
                total += weights[at : at + 1] * turned[comp * columns : (comp + 1) * columns]
            pieces.append(total)
        contribution = jnp.concatenate(pieces, axis=0).astype(BF16)
        own[...] -= dot_nt(contribution, pick[far, part])

    with jax.named_scope("wait_back"):
        arrive(BACK, recv3.at[0])
    with jax.named_scope("gather"):
        repeat(chunks, lambda part: gather_back(0, part))
    with jax.named_scope("wait_back_far"):
        arrive(BACK_FAR, recv3.at[1])
    with jax.named_scope("gather_far"):
        repeat(chunks, lambda part: gather_back(1, part))

        sketch = own[...]
        sketch_ref[...] = sketch
        flat = jnp.concatenate(
            [sketch[row * columns : (row + 1) * columns] for row in range(params)], axis=1
        )
        head = flat.astype(BF16)
        rest = (flat - head.astype(F32)).astype(BF16)
        parts = jnp.concatenate([head, rest], axis=0)
        products = dot_nt(parts, parts)
        products = products[:columns] + products[columns:]
        gsend[...] = fold(products[:, :columns]) + fold(products[:, columns:])

    def send_gram(turn):
        other = jnp.where(turn - 1 >= me, turn, turn - 1)
        remote(GRAM, gsend, grecv.at[me], other).start()

    turns(1, devices, send_gram)
    pltpu.make_async_copy(gsend, grecv.at[me], recv_sems.at[GRAM]).start()
    most = pl.ds(0, half - 1)
    sent(ASK, recv1.at[most])
    sent(ASK_FAR, recv1_far)
    sent(TABLE, far_table)
    sent(SUM, recv2.at[0, most])
    sent(SUM_FAR, recv2.at[1, most])
    sent(BACK, recv3.at[0, most])
    sent(BACK_FAR, recv3.at[1])
    with jax.named_scope("wait_gram"):
        arrive(GRAM, grecv)
    packed_ref[...] = jnp.sum(grecv[...], axis=0)

    sent(GRAM, grecv.at[pl.ds(0, devices - 1)])


def finish(
    sizes,
    sketch_ref, packed_ref,
    sketch_hbm, basis_hbm, factor_hbm,
    basis_ref, factor_ref, sems,
):
    params, columns, height = sizes
    cam_width = sketch_ref.shape[1]
    sketch_copy = pltpu.make_async_copy(sketch_ref, sketch_hbm, sems.at[0])
    sketch_copy.start()
    with jax.named_scope("eliminate"):
        gram = unfold_gram(packed_ref[...], columns) / height
        strips = columns // STRIP
        unit = jnp.where(
            rows_iota((columns, columns)) == lanes_iota((columns, columns)), 1.0, 0.0
        )
        both = jnp.concatenate([unit, gram, unit, unit], axis=1)
        work = [both[s * STRIP : (s + 1) * STRIP] for s in range(strips)]
        row_ids = rows_iota((STRIP, 1))
        roots = [jnp.zeros((STRIP, LANES), F32) for _ in range(strips)]
        def spread_columns(first, least):
            low = columns + first * STRIP
            return [
                {
                    s: jnp.broadcast_to(work[s][:, low + j : low + j + 1], (STRIP, LANES))
                    for s in range(least, strips)
                }
                for j in range(STRIP)
            ]

        panel = spread_columns(0, 0)
        for base in range(strips):
            later = spread_columns(base + 1, base + 1) if base + 1 < strips else []
            for j in range(0, STRIP, 2):
                a = panel[j][base][j : j + 1]
                b = panel[j + 1][base][j : j + 1]
                c = panel[j + 1][base][j + 1 : j + 2]
                det = a * c - b * b
                over_det, over_a = 1.0 / det, 1.0 / a
                roots[base] = jnp.where(row_ids == j, lax.rsqrt(a), roots[base])
                roots[base] = jnp.where(
                    row_ids == j + 1, lax.rsqrt(det * over_a), roots[base]
                )
                first, second, scale, by_first, by_second = {}, {}, {}, {}, {}
                for s in range(base, strips):
                    first[s] = panel[j][s] * c - panel[j + 1][s] * b
                    second[s] = panel[j + 1][s] * a - panel[j][s] * b
                    scale[s] = (
                        jnp.where(row_ids > j + 1, over_det, 0.0) if s == base else over_det
                    )
                    by_first[s] = first[s] * scale[s]
                    by_second[s] = second[s] * scale[s]
                for place, column in enumerate(later):
                    upper = panel[j][base + 1][place : place + 1]
                    lower = panel[j + 1][base + 1][place : place + 1]
                    for s in range(base + 1, strips):
                        column[s] = column[s] - (by_first[s] * upper + by_second[s] * lower)
                for column in panel[j + 2 :]:
                    upper, lower = column[base][j : j + 1], column[base][j + 1 : j + 2]
                    for s in range(base, strips):
                        column[s] = column[s] - (first[s] * upper + second[s] * lower) * scale[s]
                upper, lower = work[base][j : j + 1], work[base][j + 1 : j + 2]
                beside = jnp.where(row_ids == j + 1, b * over_a, 0.0)
                for s in range(base, strips):
                    step = by_first[s] * upper + by_second[s] * lower
                    if s == base:
                        step += beside * upper
                    work[s] = work[s] - step
            panel = later
        done = jnp.concatenate(
            [work[s] * roots[s] for s in range(strips)], axis=0
        )
        on_upper = rows_iota((columns, columns)) <= lanes_iota((columns, columns))
        factor_ref[...] = jnp.where(on_upper, done[:, columns : 2 * columns], 0.0)
    factor_copy = pltpu.make_async_copy(factor_ref, factor_hbm, sems.at[1])
    factor_copy.start()
    with jax.named_scope("basis"):
        flat = jnp.concatenate(
            [sketch_ref[row * columns : (row + 1) * columns] for row in range(params)], axis=1
        )
        head = flat.astype(BF16)
        rest = (flat - head.astype(F32)).astype(BF16)
        upper = done.astype(BF16)
        lower = (done - upper.astype(F32)).astype(BF16)
        left = jnp.where(lanes_iota(done.shape) < 3 * columns, upper, lower)
        right = jnp.concatenate([head, jnp.zeros_like(head), rest, head], axis=0)
        basis = dot(left, right)
        for row in range(params):
            basis_ref[row * columns : (row + 1) * columns, :] = basis[
                :, row * cam_width : (row + 1) * cam_width
            ]
    basis_copy = pltpu.make_async_copy(basis_ref, basis_hbm, sems.at[2])
    basis_copy.start()
    with jax.named_scope("write"):
        sketch_copy.wait()
        factor_copy.wait()
        basis_copy.wait()


def on_device(omega, u_blocks, w_blocks, v_inverse, obs_camera, obs_track, obs_mask):
    track_count = lax.axis_size("track")
    cam_count = lax.axis_size("cam")
    devices = track_count * cam_count
    half = devices // 2
    columns, params, cam_width = omega.shape
    obs_count = obs_camera.shape[0]
    tracks = v_inverse.shape[2]
    capacity = max(2, 2 * obs_count // devices)
    rows = -(-capacity // (LANES // columns) // 8) * 8
    groups = -(-capacity // rows)
    span = half
    while span * rows * groups > CHUNK and span % 2 == 0:
        span //= 2
    chunk = span * rows * groups
    chunks = half // span

    table = omega.transpose(1, 0, 2).reshape(params * columns, cam_width)
    line = (1, obs_count)
    operands = (
        table,
        u_blocks,
        w_blocks,
        v_inverse,
        obs_camera.reshape(line),
        obs_track.reshape(line),
        obs_mask.reshape(line),
    )
    sizes = (track_count, cam_count, params, columns, rows, groups, span)
    message = pltpu.VMEM((2, half, 3 * rows, LANES), BF16)
    tall = columns * columns // 2 // LANES + 1
    wide_shape = (chunks, columns, chunk)
    pick_shape = (chunks, cam_width, chunk)
    whole = jax.ShapeDtypeStruct((params * columns, cam_width), F32)
    square = jax.ShapeDtypeStruct((columns, columns), F32)
    in_vmem = pl.BlockSpec(memory_space=pltpu.VMEM)
    anywhere = pl.BlockSpec(memory_space=pl.ANY)
    sketch, packed = pl.pallas_call(
        functools.partial(kernel, sizes),
        out_shape=(
            pltpu.VMEM((params * columns, cam_width), F32),
            pltpu.VMEM((tall, LANES), F32),
        ),
        in_specs=[anywhere] * 7,
        out_specs=(in_vmem,) * 2,
        scratch_shapes=[
            pltpu.VMEM((half, 2 * rows, LANES), BF16),
            pltpu.VMEM((half, 2 * rows, LANES), BF16),
            pltpu.VMEM((half, rows, LANES), BF16),
        ]
        + [message] * 4
        + [
            pltpu.VMEM((tall, LANES), F32),
            pltpu.VMEM((devices, tall, LANES), F32),
            pltpu.VMEM((params * columns, cam_width), BF16),
            pltpu.VMEM((columns, obs_count), F32),
            pltpu.VMEM((2, chunks, tracks, chunk), BF16),
            pltpu.VMEM((2,) + wide_shape, F32),
            pltpu.VMEM((2,) + pick_shape, BF16),
            pltpu.VMEM(wide_shape, F32),
            pltpu.VMEM(pick_shape, BF16),
            pltpu.VMEM((params * columns, cam_width), F32),
            pltpu.VMEM((3 * columns, tracks), F32),
            pltpu.SemaphoreType.DMA((8,)),
            pltpu.SemaphoreType.DMA((8,)),
        ]
        + [pltpu.VMEM(array.shape, array.dtype) for array in operands]
        + [pltpu.SemaphoreType.DMA((len(operands),))],
        compiler_params=pltpu.CompilerParams(collective_id=0, has_side_effects=True),
    )(*operands)
    sketch, basis, factor = pl.pallas_call(
        functools.partial(finish, (params, columns, params * cam_width * devices)),
        out_shape=(whole, whole, square),
        in_specs=[in_vmem] * 2,
        out_specs=(anywhere,) * 3,
        scratch_shapes=[
            pltpu.VMEM((params * columns, cam_width), F32),
            pltpu.VMEM((columns, columns), F32),
            pltpu.SemaphoreType.DMA((3,)),
        ],
    )(*(pltpu.with_memory_space_constraint(x, pltpu.VMEM) for x in (sketch, packed)))

    def unfold(array):
        return array.reshape(params, columns, cam_width).transpose(1, 0, 2)

    return (unfold(sketch), unfold(basis), factor)


def solution(mesh):
    spread = P(None, None, ("track", "cam"))
    flat = P(("track", "cam"))
    return jax.shard_map(
        on_device,
        mesh=mesh,
        in_specs=(spread,) * 4 + (flat,) * 3,
        out_specs=(spread, spread, P()),
        check_vma=False,
    )
```

```python
import functools

import jax
import jax.numpy as jnp
from jax import lax
from jax.experimental import pallas as pl
from jax.experimental.pallas import tpu as pltpu
from jax.sharding import PartitionSpec as P

BLK_OBS = 128
TRK_BLK = 32
LANES = 128
STRIP = 8
CHUNK = 512
UNROLL = 32

LOGICAL = pl.DeviceIdType.LOGICAL
NT = (((1,), (1,)), ((), ()))
F32 = jnp.float32
BF16 = jnp.bfloat16

ASK, ASK_FAR, TABLE, SUM, SUM_FAR, BACK, BACK_FAR, GRAM = range(8)


def dot(left, right, precision=None):
    return jnp.dot(left, right, precision=precision, preferred_element_type=F32)


def dot_nt(left, right, precision=None):
    return lax.dot_general(left, right, NT, precision=precision, preferred_element_type=F32)


def one_hot(condition):
    return jnp.where(condition, 1.0, 0.0).astype(BF16)


def rows_iota(shape):
    return lax.broadcasted_iota(jnp.int32, shape, 0)


def lanes_iota(shape):
    return lax.broadcasted_iota(jnp.int32, shape, 1)


def turns(first, count, body):
    if count - first <= UNROLL:
        for turn in range(first, count):
            body(turn)
    else:
        pl.loop(first, count)(body)


def repeat(count, body):
    if count == 1:
        body(0)
    else:
        pl.loop(0, count)(body)


def fold(gram):
    columns = gram.shape[0]
    middle = columns // 2
    folds = LANES // columns
    tall = middle // folds
    top, bottom = gram[:middle], gram[middle:]
    first, second = [], []
    for k in range(folds):
        first.append(top[k * tall : (k + 1) * tall])
        piece = bottom[k * tall : (k + 1) * tall]
        second += [piece[:, middle:], piece[:, :middle]]
    lane = lanes_iota((tall, LANES))
    row = rows_iota((tall, LANES)) + lane // columns * tall
    packed = jnp.where(
        lax.rem(lane, columns) >= row,
        jnp.concatenate(first, axis=1),
        jnp.concatenate(second, axis=1),
    )
    shape = (middle, columns)
    on_diagonal = lanes_iota(shape) == rows_iota(shape) + middle
    diagonal = jnp.sum(jnp.where(on_diagonal, bottom, 0.0), axis=0, keepdims=True)
    diagonal = jnp.concatenate([diagonal, jnp.zeros((1, LANES - columns), F32)], axis=1)
    return jnp.concatenate([packed, diagonal], axis=0)


def unfold_gram(packed, columns):
    middle = columns // 2
    folds = LANES // columns
    tall = middle // folds
    both = jnp.concatenate(
        [packed[:tall, k * columns : (k + 1) * columns] for k in range(folds)], axis=0
    )
    gap = jnp.zeros((tall, middle), F32)
    moved = jnp.concatenate(
        [
            jnp.concatenate([gap, packed[:tall, k * columns : k * columns + middle]], axis=1)
            for k in range(folds)
        ],
        axis=0,
    )
    shape = (middle, columns)
    row, lane = rows_iota(shape), lanes_iota(shape)
    top = jnp.where(lane >= row, both, 0.0)
    bottom = jnp.where(lane < row + middle, moved, 0.0)
    bottom += jnp.where(lane == row + middle, packed[tall : tall + 1, :columns], 0.0)
    half = jnp.concatenate([top, bottom], axis=0)
    square = (columns, columns)
    wide = jnp.concatenate([half, jnp.zeros((columns, LANES - columns), F32)], axis=1)
    turned = jnp.concatenate([wide] + [jnp.zeros((LANES - columns, LANES), F32)], axis=0).T
    turned = turned[:columns, :columns]
    return half + jnp.where(lanes_iota(square) == rows_iota(square), 0.0, turned)


def kernel(
    sizes,
    omega_hbm, u_hbm, w_hbm, v_hbm, camera_hbm, track_hbm, mask_hbm,
    sketch_ref, packed_ref,
    send1, recv1, recv1_far, send2, recv2, send3, recv3, gsend, grecv, far_table,
    fields, to_track, wide, pick, far_wide, far_pick, own, sum_ref,
    send_sems, recv_sems,
    omega_ref, u_ref, w_ref, v_ref, camera_ref, track_ref, mask_ref, load_sems,
):
    track_count, cam_count, params, columns, rows, groups, span = sizes
    devices = track_count * cam_count
    half = devices // 2
    cam_width = omega_ref.shape[1]
    obs_count = camera_ref.shape[1]
    tracks = v_ref.shape[2]
    part_rows = span * rows
    chunk = groups * part_rows
    chunks = half // span
    me = lax.axis_index("track") * cam_count + lax.axis_index("cam")
    side = me // half
    place_at = me - side * half
    home = side * half
    away = half - home

    def wrapped(start, turn, count):
        place = start + turn
        return jnp.where(place >= count, place - count, place)

    barrier = pltpu.get_barrier_semaphore()

    def greet(device):
        pl.semaphore_signal(barrier, inc=1, device_id=device, device_id_type=LOGICAL)

    turns(1, half, lambda turn: greet(home + wrapped(place_at, turn, half)))
    greet(away + place_at)

    loads = [
        pltpu.make_async_copy(source, target, load_sems.at[index])
        for index, (source, target) in enumerate(
            [
                (camera_hbm, camera_ref),
                (track_hbm, track_ref),
                (mask_hbm, mask_ref),
                (w_hbm, w_ref),
                (omega_hbm, omega_ref),
                (u_hbm, u_ref),
                (v_hbm, v_ref),
            ]
        )
    ]
    for load in loads:
        load.start()

    def remote(index, src, dst, device):
        return pltpu.make_async_remote_copy(
            src_ref=src,
            dst_ref=dst,
            send_sem=send_sems.at[index],
            recv_sem=recv_sems.at[index],
            device_id=device,
            device_id_type=LOGICAL,
        )

    def to_home(index, src, dst):
        def send(turn):
            other = wrapped(place_at, turn, half)
            remote(index, src.at[other], dst.at[place_at], home + other).start()

        turns(1, half, send)
        pltpu.make_async_copy(src.at[place_at], dst.at[place_at], recv_sems.at[index]).start()

    quarter = half // 2 if half % 2 == 0 else half
    in_quarter = lax.rem(place_at, quarter)

    def far_place(turn):
        other = wrapped(in_quarter, turn % quarter, quarter)
        if quarter == half:
            return other
        return other + quarter * (1 - side + (2 * side - 1) * (turn // quarter))

    def to_away(index, src, dst):
        def send(turn):
            other = far_place(turn)
            remote(index, src(other), dst.at[place_at], away + other).start()

        turns(0, half, send)

    def arrive(index, dst):
        pltpu.make_async_copy(dst, dst, recv_sems.at[index]).wait()

    def sent(index, part):
        pltpu.make_async_copy(part, part, send_sems.at[index]).wait()

    def pack(part, values, dst, at=0):
        for index in range(values.shape[0] // columns):
            block = values[index * columns : (index + 1) * columns]
            pieces = [block[:, g * part_rows : (g + 1) * part_rows] for g in range(groups)]
            if groups * columns < LANES:
                pieces.append(jnp.zeros((LANES - groups * columns, part_rows), F32))
            turned = jnp.concatenate(pieces, axis=0).T.reshape(span, rows, LANES)
            low = at + index * rows
            dst[pl.ds(part * span, span), low : low + rows] = turned.astype(BF16)

    def unpack(part, src, at, count):
        blocks = []
        for index in range(count):
            low = at + index * rows
            block = src[pl.ds(part * span, span), low : low + rows]
            turned = block.reshape(part_rows, LANES).astype(F32).T
            blocks.append(
                jnp.concatenate(
                    [turned[g * columns : (g + 1) * columns] for g in range(groups)], axis=1
                )
            )
        return jnp.concatenate(blocks, axis=0)

    with jax.named_scope("place"):
        for load in loads[:4]:
            load.wait()
        camera = camera_ref[...]
        owner = camera // cam_width
        local = camera - owner * cam_width
        owner = owner - home
        owner = jnp.where(owner < 0, owner + devices, owner)
        track_id = lanes_iota((1, obs_count)) // BLK_OBS * TRK_BLK + track_ref[...]
        live = mask_ref[...].astype(F32)
        fields[...] = jnp.zeros_like(fields)
        for row in range(params):
            fields[3 * row : 3 * row + 3, :] = w_ref[row].astype(F32) * live
        high = local // 256
        fields[3 * params : 3 * params + 1, :] = high.astype(F32)
        fields[3 * params + 1 : 3 * params + 2, :] = (local - high * 256).astype(F32)
        owned = one_hot(rows_iota((devices, obs_count)) == owner)
        earlier = one_hot(rows_iota((obs_count, obs_count)) < lanes_iota((obs_count, obs_count)))
        ranks = dot(owned, earlier)
        rank = jnp.sum(ranks * owned.astype(F32), axis=0, keepdims=True).astype(jnp.int32)
        group = jnp.zeros_like(rank)
        for g in range(1, groups):
            group += jnp.where(rank >= g * rows, 1, 0)
        offset = group * part_rows + rank - group * rows
        member = one_hot(rows_iota((tracks, obs_count)) == track_id)
        table = jnp.concatenate([fields[...].astype(BF16), member], axis=0)

        for far in range(2):

            def place(part):
                nearby = owner - far * half - part * span
                inside = jnp.logical_and(nearby >= 0, nearby < span)
                slot = jnp.where(inside, nearby * rows + offset, -1)
                slots = one_hot(rows_iota((chunk, obs_count)) == slot)
                placed = dot_nt(table, slots)
                pack(part, placed[:columns], send1, far * rows)
                to_track[far, part] = placed[columns:].astype(BF16)

            repeat(chunks, place)

    with jax.named_scope("barrier"):
        loads[4].wait()
        pl.semaphore_wait(barrier, half)
    table_copy = remote(TABLE, omega_ref, far_table, away + place_at)
    to_home(ASK, send1, recv1)
    table_copy.start()

    with jax.named_scope("own"):
        for load in loads[5:]:
            load.wait()
        for row in range(params):
            total = jnp.zeros((columns, cam_width), F32)
            for col in range(params):
                total += u_ref[row, col : col + 1, :] * omega_ref[
                    col * columns : (col + 1) * columns, :
                ].astype(F32)
            own[row * columns : (row + 1) * columns, :] = total
        sum_ref[...] = jnp.zeros_like(sum_ref)

    def read_request(part, src, at, wide_to, pick_to):
        turned = unpack(part, src, at, 1)
        wide_to[part] = turned
        number = turned[3 * params : 3 * params + 1] * 256.0 + turned[
            3 * params + 1 : 3 * params + 2
        ]
        pick_to[part] = one_hot(rows_iota((cam_width, chunk)) == number.astype(jnp.int32))

    def project(part, cameras, weights, chosen, dst):
        gathered = dot(cameras[...], chosen[part])
        turned = weights[part]
        pieces = []
        for comp in range(3):
            total = jnp.zeros((columns, chunk), F32)
            for row in range(params):
                at = row * 3 + comp
                total += turned[at : at + 1] * gathered[row * columns : (row + 1) * columns]
            pieces.append(total)
        pack(part, jnp.concatenate(pieces, axis=0), dst)

    with jax.named_scope("wait_ask"):
        arrive(ASK, recv1)
    with jax.named_scope("project"):
        repeat(chunks, lambda part: read_request(part, recv1, 0, wide.at[0], pick.at[0]))
        repeat(chunks, lambda part: read_request(part, recv1, rows, far_wide, far_pick))
        repeat(chunks, lambda part: project(part, omega_ref, wide.at[0], pick.at[0], send2.at[0]))
    to_home(SUM, send2.at[0], recv2.at[0])
    with jax.named_scope("wait_table"):
        arrive(TABLE, far_table)
    with jax.named_scope("project_far"):
        repeat(chunks, lambda part: project(part, far_table, far_wide, far_pick, send2.at[1]))
    to_home(SUM_FAR, send2.at[1], recv2.at[1])
    to_away(ASK_FAR, lambda other: send1.at[other, pl.ds(rows, rows)], recv1_far)

    def collect(far, part):
        values = unpack(part, recv2.at[far], 0, 3).astype(BF16)
        sum_ref[...] += dot_nt(values, to_track[far, part])

    with jax.named_scope("wait_sum"):
        arrive(SUM, recv2.at[0])
    with jax.named_scope("collect"):
        repeat(chunks, lambda part: collect(0, part))
    with jax.named_scope("wait_sum_far"):
        arrive(SUM_FAR, recv2.at[1])
    with jax.named_scope("collect_far"):
        repeat(chunks, lambda part: collect(1, part))
        pieces = []
        for row in range(3):
            total = jnp.zeros((columns, tracks), F32)
            for col in range(3):
                total += v_ref[row, col : col + 1, :] * sum_ref[
                    col * columns : (col + 1) * columns
                ]
            pieces.append(total)
        solved = jnp.concatenate(pieces, axis=0).astype(BF16)
        repeat(
            chunks, lambda part: pack(part, dot(solved, to_track[1, part]), send3.at[1])
        )
    to_away(BACK_FAR, lambda other: send3.at[1, other], recv3.at[1])
    with jax.named_scope("spread"):
        repeat(
            chunks, lambda part: pack(part, dot(solved, to_track[0, part]), send3.at[0])
        )
    to_home(BACK, send3.at[0], recv3.at[0])
    with jax.named_scope("read_ask_far"):
        arrive(ASK_FAR, recv1_far)
        repeat(chunks, lambda part: read_request(part, recv1_far, 0, wide.at[1], pick.at[1]))

    def gather_back(far, part):
        turned = unpack(part, recv3.at[far], 0, 3)
        weights = wide[far, part]
        pieces = []
        for row in range(params):
            total = jnp.zeros((columns, chunk), F32)
            for comp in range(3):
                at = row * 3 + comp
                total += weights[at : at + 1] * turned[comp * columns : (comp + 1) * columns]
            pieces.append(total)
        contribution = jnp.concatenate(pieces, axis=0).astype(BF16)
        own[...] -= dot_nt(contribution, pick[far, part])

    with jax.named_scope("wait_back"):
        arrive(BACK, recv3.at[0])
    with jax.named_scope("gather"):
        repeat(chunks, lambda part: gather_back(0, part))
    with jax.named_scope("wait_back_far"):
        arrive(BACK_FAR, recv3.at[1])
    with jax.named_scope("gather_far"):
        repeat(chunks, lambda part: gather_back(1, part))

        sketch = own[...]
        sketch_ref[...] = sketch
        flat = jnp.concatenate(
            [sketch[row * columns : (row + 1) * columns] for row in range(params)], axis=1
        )
        head = flat.astype(BF16)
        rest = (flat - head.astype(F32)).astype(BF16)
        parts = jnp.concatenate([head, rest], axis=0)
        products = dot_nt(parts, parts)
        products = products[:columns] + products[columns:]
        gsend[...] = fold(products[:, :columns]) + fold(products[:, columns:])

    def send_gram(turn):
        other = jnp.where(turn - 1 >= me, turn, turn - 1)
        remote(GRAM, gsend, grecv.at[me], other).start()

    turns(1, devices, send_gram)
    pltpu.make_async_copy(gsend, grecv.at[me], recv_sems.at[GRAM]).start()
    most = pl.ds(0, half - 1)
    sent(ASK, recv1.at[most])
    sent(ASK_FAR, recv1_far)
    sent(TABLE, far_table)
    sent(SUM, recv2.at[0, most])
    sent(SUM_FAR, recv2.at[1, most])
    sent(BACK, recv3.at[0, most])
    sent(BACK_FAR, recv3.at[1])
    with jax.named_scope("wait_gram"):
        arrive(GRAM, grecv)
    total = grecv[...]
    while total.shape[0] % 2 == 0:
        middle = total.shape[0] // 2
        total = total[:middle] + total[middle:]
    packed_ref[...] = jnp.sum(total, axis=0)

    sent(GRAM, grecv.at[pl.ds(0, devices - 1)])


def finish(
    sizes,
    sketch_ref, packed_ref,
    sketch_hbm, basis_hbm, factor_hbm,
    basis_ref, factor_ref, sems,
):
    params, columns, height = sizes
    cam_width = sketch_ref.shape[1]
    sketch_copy = pltpu.make_async_copy(sketch_ref, sketch_hbm, sems.at[0])
    sketch_copy.start()
    with jax.named_scope("eliminate"):
        gram = unfold_gram(packed_ref[...] * (1.0 / height), columns)
        strips = columns // STRIP
        unit = jnp.where(
            rows_iota((columns, columns)) == lanes_iota((columns, columns)), 1.0, 0.0
        )
        both = jnp.concatenate([unit, gram, unit, unit], axis=1)
        work = [both[s * STRIP : (s + 1) * STRIP] for s in range(strips)]
        row_ids = rows_iota((STRIP, 1))
        roots = [jnp.zeros((STRIP, LANES), F32) for _ in range(strips)]
        def spread_columns(first, least):
            low = columns + first * STRIP
            return [
                {
                    s: jnp.broadcast_to(work[s][:, low + j : low + j + 1], (STRIP, LANES))
                    for s in range(least, strips)
                }
                for j in range(STRIP)
            ]

        panel = spread_columns(0, 0)
        for base in range(strips):
            later = spread_columns(base + 1, base + 1) if base + 1 < strips else []
            for j in range(0, STRIP, 2):
                a = panel[j][base][j : j + 1]
                b = panel[j + 1][base][j : j + 1]
                c = panel[j + 1][base][j + 1 : j + 2]
                det = a * c - b * b
                over_det, over_a = 1.0 / det, 1.0 / a
                roots[base] = jnp.where(row_ids == j, lax.rsqrt(a), roots[base])
                roots[base] = jnp.where(
                    row_ids == j + 1, lax.rsqrt(det * over_a), roots[base]
                )
                first, second, scale, by_first, by_second = {}, {}, {}, {}, {}
                for s in range(base, strips):
                    first[s] = panel[j][s] * c - panel[j + 1][s] * b
                    second[s] = panel[j + 1][s] * a - panel[j][s] * b
                    scale[s] = (
                        jnp.where(row_ids > j + 1, over_det, 0.0) if s == base else over_det
                    )
                    by_first[s] = first[s] * scale[s]
                    by_second[s] = second[s] * scale[s]
                for place, column in enumerate(later):
                    upper = panel[j][base + 1][place : place + 1]
                    lower = panel[j + 1][base + 1][place : place + 1]
                    for s in range(base + 1, strips):
                        column[s] = column[s] - (by_first[s] * upper + by_second[s] * lower)
                for column in panel[j + 2 :]:
                    upper, lower = column[base][j : j + 1], column[base][j + 1 : j + 2]
                    for s in range(base, strips):
                        column[s] = column[s] - (first[s] * upper + second[s] * lower) * scale[s]
                upper, lower = work[base][j : j + 1], work[base][j + 1 : j + 2]
                beside = jnp.where(row_ids == j + 1, b * over_a, 0.0)
                for s in range(base, strips):
                    step = by_first[s] * upper + by_second[s] * lower
                    if s == base:
                        step += beside * upper
                    work[s] = work[s] - step
            panel = later
        done = jnp.concatenate(
            [work[s] * roots[s] for s in range(strips)], axis=0
        )
        on_upper = rows_iota((columns, columns)) <= lanes_iota((columns, columns))
        factor_ref[...] = jnp.where(on_upper, done[:, columns : 2 * columns], 0.0)
    factor_copy = pltpu.make_async_copy(factor_ref, factor_hbm, sems.at[1])
    factor_copy.start()
    with jax.named_scope("basis"):
        flat = jnp.concatenate(
            [sketch_ref[row * columns : (row + 1) * columns] for row in range(params)], axis=1
        )
        head = flat.astype(BF16)
        rest = (flat - head.astype(F32)).astype(BF16)
        upper = done.astype(BF16)
        lower = (done - upper.astype(F32)).astype(BF16)
        left = jnp.where(lanes_iota(done.shape) < 3 * columns, upper, lower)
        right = jnp.concatenate([head, jnp.zeros_like(head), rest, head], axis=0)
        basis = dot(left, right)
        for row in range(params):
            basis_ref[row * columns : (row + 1) * columns, :] = basis[
                :, row * cam_width : (row + 1) * cam_width
            ]
    basis_copy = pltpu.make_async_copy(basis_ref, basis_hbm, sems.at[2])
    basis_copy.start()
    with jax.named_scope("write"):
        sketch_copy.wait()
        factor_copy.wait()
        basis_copy.wait()


def on_device(omega, u_blocks, w_blocks, v_inverse, obs_camera, obs_track, obs_mask):
    track_count = lax.axis_size("track")
    cam_count = lax.axis_size("cam")
    devices = track_count * cam_count
    half = devices // 2
    columns, params, cam_width = omega.shape
    obs_count = obs_camera.shape[0]
    tracks = v_inverse.shape[2]
    capacity = max(2, 2 * obs_count // devices)
    rows = -(-capacity // (LANES // columns) // 8) * 8
    groups = -(-capacity // rows)
    span = half
    while span * rows * groups > CHUNK and span % 2 == 0:
        span //= 2
    chunk = span * rows * groups
    chunks = half // span

    table = omega.transpose(1, 0, 2).reshape(params * columns, cam_width)
    line = (1, obs_count)
    operands = (
        table,
        u_blocks,
        w_blocks,
        v_inverse,
        obs_camera.reshape(line),
        obs_track.reshape(line),
        obs_mask.reshape(line),
    )
    sizes = (track_count, cam_count, params, columns, rows, groups, span)
    message = pltpu.VMEM((2, half, 3 * rows, LANES), BF16)
    tall = columns * columns // 2 // LANES + 1
    wide_shape = (chunks, columns, chunk)
    pick_shape = (chunks, cam_width, chunk)
    whole = jax.ShapeDtypeStruct((params * columns, cam_width), F32)
    square = jax.ShapeDtypeStruct((columns, columns), F32)
    in_vmem = pl.BlockSpec(memory_space=pltpu.VMEM)
    anywhere = pl.BlockSpec(memory_space=pl.ANY)
    sketch, packed = pl.pallas_call(
        functools.partial(kernel, sizes),
        out_shape=(
            pltpu.VMEM((params * columns, cam_width), F32),
            pltpu.VMEM((tall, LANES), F32),
        ),
        in_specs=[anywhere] * 7,
        out_specs=(in_vmem,) * 2,
        scratch_shapes=[
            pltpu.VMEM((half, 2 * rows, LANES), BF16),
            pltpu.VMEM((half, 2 * rows, LANES), BF16),
            pltpu.VMEM((half, rows, LANES), BF16),
        ]
        + [message] * 4
        + [
            pltpu.VMEM((tall, LANES), F32),
            pltpu.VMEM((devices, tall, LANES), F32),
            pltpu.VMEM((params * columns, cam_width), BF16),
            pltpu.VMEM((columns, obs_count), F32),
            pltpu.VMEM((2, chunks, tracks, chunk), BF16),
            pltpu.VMEM((2,) + wide_shape, F32),
            pltpu.VMEM((2,) + pick_shape, BF16),
            pltpu.VMEM(wide_shape, F32),
            pltpu.VMEM(pick_shape, BF16),
            pltpu.VMEM((params * columns, cam_width), F32),
            pltpu.VMEM((3 * columns, tracks), F32),
            pltpu.SemaphoreType.DMA((8,)),
            pltpu.SemaphoreType.DMA((8,)),
        ]
        + [pltpu.VMEM(array.shape, array.dtype) for array in operands]
        + [pltpu.SemaphoreType.DMA((len(operands),))],
        compiler_params=pltpu.CompilerParams(collective_id=0, has_side_effects=True),
    )(*operands)
    sketch, basis, factor = pl.pallas_call(
        functools.partial(finish, (params, columns, params * cam_width * devices)),
        out_shape=(whole, whole, square),
        in_specs=[in_vmem] * 2,
        out_specs=(anywhere,) * 3,
        scratch_shapes=[
            pltpu.VMEM((params * columns, cam_width), F32),
            pltpu.VMEM((columns, columns), F32),
            pltpu.SemaphoreType.DMA((3,)),
        ],
    )(*(pltpu.with_memory_space_constraint(x, pltpu.VMEM) for x in (sketch, packed)))

    def unfold(array):
        return array.reshape(params, columns, cam_width).transpose(1, 0, 2)

    return (unfold(sketch), unfold(basis), factor)


def solution(mesh):
    spread = P(None, None, ("track", "cam"))
    flat = P(("track", "cam"))
    return jax.shard_map(
        on_device,
        mesh=mesh,
        in_specs=(spread,) * 4 + (flat,) * 3,
        out_specs=(spread, spread, P()),
        check_vma=False,
    )
```
